128 devices in a mesh: ta: 16 (over z_hi, y, core), gx: 8 (over x, z_lo).
Axes of the slice: x: 4, y: 4, z: 4 (z_hi: 2, z_lo: 2; z = z_hi * 2 + z_lo), core: 2. Of those that a mesh axis runs over, the one named last changes fastest.
Arguments:
- eigenvectors: bfloat16 [16, 2, 32768, 3, 192], P('ta', None, 'gx'), may hold values from -6 to 6
- site_index: int32 [32768], P('gx'), may hold values from 0 to 32767, each once
- momenta: int32 [2, 3], replicated, may hold values from -3 to 3
- perambulators: bfloat16 [2, 16, 16, 768, 768], P(None, 'gx', 'ta'), may hold values from -6 to 6
- spin_perm: int32 [2, 4], replicated, may hold values from 0 to 3, each once within a row
- spin_sign: int32 [2, 4], replicated, may hold values from 0 to 1
Outputs:
- forward_box: bfloat16 [2, 16, 16, 768, 768], P(None, 'gx', 'ta')
- backward_box: bfloat16 [2, 16, 16, 768, 768], P(None, 'gx', 'ta')
The draws below stay inside these ranges and needn't reach their ends.
Inputs may be any that keep to these rules, and one draw needn't show every extreme that they name: `site_index`: each lattice site appears exactly once. `spin_perm`: each row is a permutation of the spins.
All inputs are finite; a program needn't handle non-finite values.
Results may differ from the reference program's by a relative error of at most 0.008.
Values may be sent and summed in bfloat16 or wider, within the bound.
A program may use at most 128 MiB of HBM per device.

```python
import math
import jax
import jax.numpy as jnp
from jax import lax

L = 32
NT = 16
NEV = 192
COLOR = 3
SPIN = 4
MOMENTA = 2
SITES = 32768
NDIM = 768


def touch_ends(drawn, rng, least, top_value):
    spot = [jax.random.randint(jax.random.fold_in(rng, axis), (), 0, length) for axis, length in enumerate(drawn.shape)]
    widest = drawn.shape.index(max(drawn.shape))
    next_to = spot[:widest] + [(spot[widest] + 1) % drawn.shape[widest]] + spot[widest + 1:]
    return drawn.at[tuple(spot)].set(least).at[tuple(next_to)].set(top_value)


def levels(own_key, extent, cuts, smallest, largest):
    factor_of = 1.0
    for position, blocks in cuts:
        draws = jax.random.uniform(jax.random.fold_in(jax.random.fold_in(own_key, 6), position), (blocks,), jnp.float32, smallest / len(cuts), largest / len(cuts))
        factor_of = factor_of * jnp.repeat(jnp.exp(draws), extent[position] // blocks).reshape((-1,) + (1,) * (len(extent) - 1 - position))
    return factor_of


def gaussian(rng, extent, width, bound, split=(), kind=jnp.bfloat16):
    array = width * jax.random.normal(rng, extent, jnp.float32)
    if split:
        array = array * levels(rng, extent, split, -0.22, 0.18)
    return jnp.clip(array, -bound, bound).astype(kind)


def setup_inputs(seed: int = 0) -> dict:
    seeds = jax.random.split(jax.random.key(seed), 7)
    eigenvectors = gaussian(seeds[0], (NT, 2, SITES, COLOR, NEV), 1.0, 6.0, ((0, 16), (2, 8)))
    site_index = jax.random.permutation(seeds[1], SITES).astype(jnp.int32)
    momenta = touch_ends(jax.random.randint(seeds[2], (MOMENTA, 3), -3, 4), jax.random.fold_in(seeds[2], 1), -3, 3).astype(jnp.int32)
    perambulators = gaussian(seeds[3], (2, NT, NT, NDIM, NDIM), 1.0, 6.0, ((1, 8), (2, 16)))
    spin_perm = jax.vmap(lambda own: jax.random.permutation(own, SPIN))(jax.random.split(seeds[4], MOMENTA)).reshape((MOMENTA, SPIN)).astype(jnp.int32)
    spin_sign = touch_ends(jax.random.randint(seeds[5], (MOMENTA, SPIN), 0, 2), jax.random.fold_in(seeds[5], 1), 0, 1).astype(jnp.int32)
    return {"eigenvectors": eigenvectors, "site_index": site_index, "momenta": momenta, "perambulators": perambulators, "spin_perm": spin_perm, "spin_sign": spin_sign}


def phases(site_index, momenta):
    first_coord = site_index // (L * L)
    second = site_index // L % L
    third_coord = site_index % L
    dotted = momenta[:, 0:1] * first_coord[None, :] + momenta[:, 1:2] * second[None, :] + momenta[:, 2:3] * third_coord[None, :]
    angles = jnp.mod(dotted, L).astype(jnp.float32) * (2.0 * math.pi / L)
    return (jnp.cos(angles), jnp.sin(angles))

def inner_rows(first_op, second_op):
    return lax.dot_general(first_op, second_op, (((0, 1), (0, 1)), ((), ())), preferred_element_type=jnp.float32)

def project(vectors, cosine, sine_value):
    real_part = vectors[0].astype(jnp.float32)
    imag_part = vectors[1].astype(jnp.float32)
    results = []
    for momentum in range(cosine.shape[0]):
        cosine_now = cosine[momentum][:, None, None]
        sine_now = sine_value[momentum][:, None, None]
        turned_real = (cosine_now * real_part - sine_now * imag_part).astype(jnp.bfloat16)
        turned_imag = (cosine_now * imag_part + sine_now * real_part).astype(jnp.bfloat16)
        real_out = inner_rows(vectors[0], turned_real) + inner_rows(vectors[1], turned_imag)
        imag_out = inner_rows(vectors[0], turned_imag) - inner_rows(vectors[1], turned_real)
        results.append(jnp.stack([real_out, imag_out]))
    return jnp.stack(results)

def spin_tables(spin_perm, spin_sign):
    spin_count = spin_perm.shape[1]
    matches = (spin_perm[:, :, None] == jnp.arange(spin_count, dtype=jnp.int32)[None, None, :]).astype(jnp.float32)
    return matches * (2 * spin_sign - 1).astype(jnp.float32)[:, :, None]

def contract(form, first_op, second_op):
    return jnp.einsum(form, first_op.astype(jnp.float32), second_op.astype(jnp.float32))

def complex_table(matrix):
    return jnp.stack([jnp.stack([matrix[0], -matrix[1]]), jnp.stack([matrix[1], matrix[0]])])

def pair_blocks(peram_block, sink_elems, source_elems, tables):
    spin_count = tables.shape[1]
    vector_count = sink_elems.shape[-1]
    dimension = spin_count * vector_count
    chiral = jnp.where(jnp.arange(spin_count) < spin_count // 2, 1.0, -1.0).astype(jnp.float32)
    blocks = peram_block.reshape(2, spin_count, vector_count, dimension)
    stacked = []
    for first_vertex, second_vertex in ((0, 1), (1, 0)):
        mixed_rows = contract('rs,cslj->crlj', tables[first_vertex].astype(jnp.bfloat16), blocks).astype(jnp.bfloat16)
        left_side = contract('ockl,cslj->oskj', complex_table(sink_elems[first_vertex]), mixed_rows).astype(jnp.bfloat16)
        left_side = left_side.reshape(2, dimension, spin_count, vector_count)
        signed = (tables[second_vertex] * chiral[None, :]).astype(jnp.bfloat16)
        turned = contract('cisk,sr->cirk', left_side, signed).astype(jnp.bfloat16)
        product = contract('cisk,ockl->oisl', turned, complex_table(source_elems[second_vertex])).astype(jnp.bfloat16)
        product = product.reshape(2, dimension, dimension)
        stacked.append(jnp.stack([product, jnp.stack([product[1], -product[0]])]))
    both_ways = jnp.stack(stacked)
    closed = contract('docim,cjm->doij', both_ways, peram_block)
    weights = jnp.repeat(chiral, vector_count) * (0.5 / math.sqrt(dimension))
    return (closed * weights).astype(jnp.bfloat16)

def reference(eigenvectors, site_index, momenta, perambulators, spin_perm, spin_sign):
    cosine, sine_value = phases(site_index, momenta)
    norm_factor = 0.5 / math.sqrt(COLOR * SITES * NEV)

    def one_time(vectors):
        return (project(vectors, cosine, sine_value) * norm_factor).astype(jnp.bfloat16)
    elementals = lax.map(one_time, eigenvectors)
    tables = spin_tables(spin_perm, spin_sign)

    def one_pair(pair_index):
        sink_time = pair_index // NT
        source_time = pair_index % NT
        peram_block = perambulators[:, sink_time, source_time]
        return pair_blocks(peram_block, elementals[sink_time], elementals[source_time], tables)
    blocks = lax.map(one_pair, jnp.arange(NT * NT, dtype=jnp.int32))
    blocks = blocks.reshape(NT, NT, 2, 2, NDIM, NDIM).transpose(2, 3, 0, 1, 4, 5)
    return (blocks[0], blocks[1])
```

```python
import functools
import math

import jax
import jax.numpy as jnp
from jax import lax
from jax.experimental import pallas as pl
from jax.experimental.pallas import tpu as pltpu
from jax.sharding import PartitionSpec as P

L = 32
NEV = 192
COLOR = 3
SPIN = 4
SITES = 32768
NDIM = SPIN * NEV
PAIR = 2 * NEV
MESH = pl.DeviceIdType.MESH
F32 = jnp.float32
BF16 = jnp.bfloat16
NT = (((1,), (1,)), ((), ()))
NN = (((1,), (0,)), ((), ()))


def dot(a, b, dims=NN):
    return lax.dot_general(a, b, dims, preferred_element_type=F32)


def project_kernel(chunk, mom_ref, site_ref, vec_ref, out_ref, acc_ref, turned_ref):
    step = pl.program_id(0)
    last = pl.num_programs(0) - 1

    @pl.when(step == 0)
    def _():
        acc_ref[...] = jnp.zeros_like(acc_ref)

    site = site_ref[...]
    first, second, third = site >> 10, (site >> 5) & (L - 1), site & (L - 1)
    real = vec_ref[0, 0].astype(F32)
    imag = vec_ref[1, 0].astype(F32)
    for p in range(2):
        dotted = mom_ref[p, 0] * first + mom_ref[p, 1] * second + mom_ref[p, 2] * third
        angle = (dotted & (L - 1)).astype(F32) * (2.0 * math.pi / L)
        cosine, sine = jnp.cos(angle), jnp.sin(angle)
        turned_ref[p * NEV : (p + 1) * NEV] = (cosine * real - sine * imag).astype(BF16)
        turned_ref[PAIR + p * NEV : PAIR + (p + 1) * NEV] = (cosine * imag + sine * real).astype(BF16)
    plain = jnp.concatenate([vec_ref[0, 0], vec_ref[1, 0]], axis=0)
    acc_ref[...] += dot(plain, turned_ref[...], NT)

    @pl.when(step == last)
    def _():
        norm = 0.5 / math.sqrt(COLOR * SITES * NEV)
        out_ref[0:NEV] = ((acc_ref[0:NEV, 0:PAIR] + acc_ref[NEV:PAIR, PAIR:NDIM]) * norm).astype(BF16)
        out_ref[NEV:PAIR] = ((acc_ref[0:NEV, PAIR:NDIM] - acc_ref[NEV:PAIR, 0:PAIR]) * norm).astype(BF16)


def project(vectors, site_index, momenta, chunk=1024, interpret=False):
    sites = vectors.shape[-1]
    cuts = sites // chunk
    return pl.pallas_call(
        functools.partial(project_kernel, chunk),
        out_shape=jax.ShapeDtypeStruct((PAIR, PAIR), BF16),
        grid=(COLOR * cuts,),
        in_specs=[
            pl.BlockSpec(memory_space=pltpu.SMEM),
            pl.BlockSpec((1, chunk), lambda i: (0, i % cuts)),
            pl.BlockSpec((2, 1, NEV, chunk), lambda i: (0, i // cuts, 0, i % cuts)),
        ],
        out_specs=pl.BlockSpec((PAIR, PAIR), lambda i: (0, 0)),
        scratch_shapes=[pltpu.VMEM((PAIR, NDIM), F32), pltpu.VMEM((NDIM, chunk), BF16)],
        compiler_params=pltpu.CompilerParams(
            dimension_semantics=("arbitrary",), vmem_limit_bytes=56 * 1024 * 1024
        ),
        cost_estimate=pl.CostEstimate(
            flops=2 * PAIR * NDIM * COLOR * sites, bytes_accessed=4 * NEV * COLOR * sites, transcendentals=0
        ),
        name="project",
        interpret=interpret,
    )(momenta, site_index, vectors)


def sum_kernel(count, part_ref, out_ref, held, send_sem, recv_sem, back_send, back_recv):
    me = lax.axis_index("gx")
    barrier = pltpu.get_barrier_semaphore()
    for hop in range(1, count):
        pl.semaphore_signal(
            barrier, inc=1, device_id={"gx": lax.rem(me + hop, count)}, device_id_type=MESH
        )
    pl.semaphore_wait(barrier, count - 1)
    copies = []
    for hop in range(1, count):
        peer = lax.rem(me + hop, count)
        copy = pltpu.make_async_remote_copy(
            src_ref=part_ref.at[peer],
            dst_ref=held.at[hop],
            send_sem=send_sem.at[hop],
            recv_sem=recv_sem.at[hop],
            device_id={"gx": peer},
            device_id_type=MESH,
        )
        copy.start()
        copies.append(copy)
    total = part_ref[me].astype(F32)
    for hop in range(1, count):
        copies[hop - 1].wait_recv()
        total = total + held[hop].astype(F32)
    out_ref[me] = total.astype(BF16)
    backs = []
    for hop in range(1, count):
        back = pltpu.make_async_remote_copy(
            src_ref=out_ref.at[me],
            dst_ref=out_ref.at[me],
            send_sem=back_send.at[hop],
            recv_sem=back_recv.at[hop],
            device_id={"gx": lax.rem(me + hop, count)},
            device_id_type=MESH,
        )
        back.start()
        backs.append(back)
    for hop in range(1, count):
        copies[hop - 1].wait_send()
        backs[hop - 1].wait()


def sum_over_sites(partial, count):
    rows = PAIR // count
    shape = (count, rows, PAIR)
    summed = pl.pallas_call(
        functools.partial(sum_kernel, count),
        out_shape=jax.ShapeDtypeStruct(shape, BF16),
        in_specs=[pl.BlockSpec(memory_space=pltpu.VMEM)],
        out_specs=pl.BlockSpec(memory_space=pltpu.VMEM),
        scratch_shapes=[pltpu.VMEM(shape, BF16)] + [pltpu.SemaphoreType.DMA((count,))] * 4,
        compiler_params=pltpu.CompilerParams(
            collective_id=0, has_side_effects=True, vmem_limit_bytes=8 * 1024 * 1024
        ),
        name="sum_over_sites",
    )(partial.reshape(shape))
    return summed.reshape(PAIR, PAIR)


def close_kernel(rows, perm_ref, sign_ref, elem_ref, tau_ref, out_ref, table, spins, turned, mixed):
    pair, block = pl.program_id(0), pl.program_id(1)

    @pl.when((pair == 0) & (block == 0))
    def _():
        table[0:NEV, 0:PAIR] = elem_ref[0:NEV]
        table[0:NEV, PAIR:NDIM] = elem_ref[NEV:PAIR]
        table[NEV:PAIR, 0:PAIR] = -elem_ref[NEV:PAIR]
        table[NEV:PAIR, PAIR:NDIM] = elem_ref[0:NEV]

    @pl.when(block == 0)
    def _():
        for a in range(SPIN):
            cut = slice(a * NEV, (a + 1) * NEV)
            spins[a, :, 0:NEV] = tau_ref[0, 0, 0, :, cut]
            spins[a, :, NEV:PAIR] = tau_ref[1, 0, 0, :, cut]
        for q in range(2):
            for a in range(SPIN):
                into = perm_ref[q, a]
                sign = (2 * sign_ref[q, a] - 1) * jnp.where(into < SPIN // 2, 1, -1)
                moved = spins[into] * sign.astype(F32).astype(BF16)
                turned[q, 0, :, a * NEV : (a + 1) * NEV] = moved[:, 0:NEV]
                turned[q, 1, :, a * NEV : (a + 1) * NEV] = moved[:, NEV:PAIR]

    start = pl.multiple_of(block * rows, rows)
    for a in range(SPIN):
        product = dot(spins[a, pl.ds(start, rows), :], table[...]).astype(BF16)
        for c in range(2):
            for q in range(2):
                left = c * PAIR + q * NEV
                mixed[q, c, :, a * NEV : (a + 1) * NEV] = product[:, left : left + NEV]
    for q in range(2):
        real, imag = mixed[q, 0], mixed[q, 1]
        out_ref[q, 0, 0] = (dot(real, turned[q, 0], NT) + dot(imag, turned[q, 1], NT)).astype(BF16)
        out_ref[q, 1, 0] = (dot(imag, turned[q, 0], NT) - dot(real, turned[q, 1], NT)).astype(BF16)


def close_pairs(peram, elem, spin_perm, spin_sign, rows=384, interpret=False):
    sinks = peram.shape[1]
    return pl.pallas_call(
        functools.partial(close_kernel, rows),
        out_shape=jax.ShapeDtypeStruct((2, 2, sinks, NDIM, NDIM), BF16),
        grid=(sinks, NDIM // rows),
        in_specs=[
            pl.BlockSpec(memory_space=pltpu.SMEM),
            pl.BlockSpec(memory_space=pltpu.SMEM),
            pl.BlockSpec((PAIR, PAIR), lambda i, j: (0, 0)),
            pl.BlockSpec((2, 1, 1, NDIM, NDIM), lambda i, j: (0, i, 0, 0, 0)),
        ],
        out_specs=pl.BlockSpec((2, 2, 1, rows, NDIM), lambda i, j: (0, 0, i, j, 0)),
        scratch_shapes=[
            pltpu.VMEM((PAIR, NDIM), BF16),
            pltpu.VMEM((SPIN, NDIM, PAIR), BF16),
            pltpu.VMEM((2, 2, NDIM, NDIM), BF16),
            pltpu.VMEM((2, 2, rows, NDIM), BF16),
        ],
        compiler_params=pltpu.CompilerParams(
            dimension_semantics=("arbitrary", "arbitrary"), vmem_limit_bytes=48 * 1024 * 1024
        ),
        cost_estimate=pl.CostEstimate(
            flops=sinks * (16 * NDIM**3 + 16 * NDIM * NDIM * NEV),
            bytes_accessed=sinks * 12 * NDIM * NDIM,
            transcendentals=0,
        ),
        name="close_pairs",
        interpret=interpret,
    )(spin_perm, spin_sign, elem, peram)


def apply_kernel(swap_ref, perm_ref, sign_ref, even_ref, odd_ref, x_ref, out0_ref, out1_ref, table):
    pair = pl.program_id(0)
    first = (pair == 0) == (swap_ref[0] == 0)
    elem = jnp.where(first, even_ref[...], odd_ref[...])
    chiral = jnp.where(lax.broadcasted_iota(jnp.int32, (1, NDIM), 1) < NDIM // 2, 1.0, -1.0)
    weights = chiral * (0.5 / math.sqrt(NDIM))
    for d in range(2):
        real = elem[0:NEV, d * NEV : (d + 1) * NEV]
        imag = elem[NEV:PAIR, d * NEV : (d + 1) * NEV]
        table[0:NEV, 0:NEV] = real
        table[0:NEV, NEV:PAIR] = -imag
        table[NEV:PAIR, 0:NEV] = imag
        table[NEV:PAIR, NEV:PAIR] = real
        out_ref = out0_ref if d == 0 else out1_ref
        for r in range(SPIN):
            start = pl.multiple_of(perm_ref[d, r] * NEV, NEV)
            sign = (2 * sign_ref[d, r] - 1).astype(F32)
            stacked = jnp.concatenate(
                [x_ref[1 - d, 0, 0, pl.ds(start, NEV), :], x_ref[1 - d, 1, 0, pl.ds(start, NEV), :]], axis=0
            )
            done = dot(table[...], stacked) * (weights * sign)
            out_ref[0, 0, 0, r * NEV : (r + 1) * NEV] = done[0:NEV].astype(BF16)
            out_ref[1, 0, 0, r * NEV : (r + 1) * NEV] = done[NEV:PAIR].astype(BF16)


def apply_sinks(swap, even, odd, blocks, spin_perm, spin_sign, interpret=False):
    sinks = blocks.shape[2]
    shape = jax.ShapeDtypeStruct((2, sinks, 1, NDIM, NDIM), BF16)
    out_spec = pl.BlockSpec((2, 1, 1, NDIM, NDIM), lambda i: (0, i, 0, 0, 0))
    smem = pl.BlockSpec(memory_space=pltpu.SMEM)
    whole = pl.BlockSpec((PAIR, PAIR), lambda i: (0, 0))
    return pl.pallas_call(
        apply_kernel,
        out_shape=(shape, shape),
        grid=(sinks,),
        in_specs=[
            smem,
            smem,
            smem,
            whole,
            whole,
            pl.BlockSpec((2, 2, 1, NDIM, NDIM), lambda i: (0, 0, i, 0, 0)),
        ],
        out_specs=(out_spec, out_spec),
        scratch_shapes=[pltpu.VMEM((PAIR, PAIR), BF16)],
        compiler_params=pltpu.CompilerParams(
            dimension_semantics=("arbitrary",), vmem_limit_bytes=48 * 1024 * 1024
        ),
        cost_estimate=pl.CostEstimate(
            flops=sinks * 16 * NDIM * NDIM * NEV, bytes_accessed=sinks * 16 * NDIM * NDIM, transcendentals=0
        ),
        name="apply_sinks",
        interpret=interpret,
    )(swap, spin_perm, spin_sign, even, odd, blocks)


def on_device(times, sites, eigenvectors, site_index, momenta, perambulators, spin_perm, spin_sign):
    vectors = jnp.transpose(eigenvectors[0], (0, 2, 3, 1))
    partial = project(vectors, site_index.reshape(1, -1), momenta)
    elem = sum_over_sites(partial, sites)
    sinks = times // sites
    moved = []
    for turn in range(sinks):
        route = []
        for t in range(times):
            for g in range(sites):
                target = g + sites * ((t + turn) % sinks)
                route.append((t * sites + g, target * sites + t // sinks))
        moved.append(lax.ppermute(elem, ("ta", "gx"), route))
    blocks = close_pairs(perambulators, elem, spin_perm, spin_sign)
    swap = (lax.axis_index("ta") // sites).astype(jnp.int32).reshape(1)
    return apply_sinks(swap, moved[0], moved[1], blocks, spin_perm, spin_sign)


def solution(mesh):
    return jax.shard_map(
        functools.partial(on_device, mesh.shape["ta"], mesh.shape["gx"]),
        mesh=mesh,
        in_specs=(
            P("ta", None, "gx", None, None),
            P("gx"),
            P(),
            P(None, "gx", "ta", None, None),
            P(),
            P(),
        ),
        out_specs=(P(None, "gx", "ta", None, None), P(None, "gx", "ta", None, None)),
        check_vma=False,
    )
```

```python
import functools
import math

import jax
import jax.numpy as jnp
from jax import lax
from jax.experimental import pallas as pl
from jax.experimental.pallas import tpu as pltpu
from jax.sharding import PartitionSpec as P

L = 32
NEV = 192
COLOR = 3
SPIN = 4
SITES = 32768
NDIM = SPIN * NEV
PAIR = 2 * NEV
LANE = 128
DEPTH = 4
MESH = pl.DeviceIdType.MESH
F32 = jnp.float32
BF16 = jnp.bfloat16
NT = (((1,), (1,)), ((), ()))
NN = (((1,), (0,)), ((), ()))


def dot(a, b, dims=NN):
    return lax.dot_general(a, b, dims, preferred_element_type=F32)


def load_phases(mom_ref, site_ref, phase):
    site = site_ref[...]
    first, second, third = site >> 10, (site >> 5) & (L - 1), site & (L - 1)
    for p in range(2):
        dotted = mom_ref[p, 0] * first + mom_ref[p, 1] * second + mom_ref[p, 2] * third
        angle = (dotted & (L - 1)).astype(F32) * (2.0 * math.pi / L)
        phase[2 * p] = jnp.cos(angle)
        phase[2 * p + 1] = jnp.sin(angle)


def project_chunk(vec, phase, cut, turned, acc, lanes):
    for j in range(lanes // LANE):
        span = slice(j * LANE, (j + 1) * LANE)
        real = vec[0, :, span].astype(F32)
        imag = vec[1, :, span].astype(F32)
        for p in range(2):
            cosine = phase[2 * p, cut, j : j + 1, :]
            sine = phase[2 * p + 1, cut, j : j + 1, :]
            turned[p * NEV : (p + 1) * NEV, span] = (cosine * real - sine * imag).astype(BF16)
            turned[PAIR + p * NEV : PAIR + (p + 1) * NEV, span] = (cosine * imag + sine * real).astype(BF16)
    plain = jnp.concatenate([vec[0], vec[1]], axis=0)
    acc[...] += dot(plain, turned[...], NT)


def arrange(pair, perm_ref, sign_ref, tau, spins, moved):
    for a in range(SPIN):
        cut = slice(a * NEV, (a + 1) * NEV)
        spins[pair, a, :, 0:NEV] = tau[0, pair, :, cut]
        spins[pair, a, :, NEV:PAIR] = tau[1, pair, :, cut]
    for q in range(2):
        for a in range(SPIN):
            into = perm_ref[q, a]
            sign = (2 * sign_ref[q, a] - 1) * jnp.where(into < SPIN // 2, 1, -1)
            block = spins[pair, into] * sign.astype(F32).astype(BF16)
            moved[pair, q, 0, :, a * NEV : (a + 1) * NEV] = block[:, 0:NEV]
            moved[pair, q, 1, :, a * NEV : (a + 1) * NEV] = block[:, NEV:PAIR]


def close_rows(pair, start, rows, table, spins, moved, mixed, out_ref):
    for a in range(SPIN):
        product = dot(spins[pair, a, pl.ds(start, rows), :], table[...]).astype(BF16)
        for c in range(2):
            for q in range(2):
                left = c * PAIR + q * NEV
                mixed[q, c, :, a * NEV : (a + 1) * NEV] = product[:, left : left + NEV]
    for q in range(2):
        real, imag = mixed[q, 0], mixed[q, 1]
        keep = pl.ds(start, rows)
        out_ref[q, 0, pair, keep, :] = (dot(real, moved[pair, q, 0], NT) + dot(imag, moved[pair, q, 1], NT)).astype(BF16)
        out_ref[q, 1, pair, keep, :] = (dot(imag, moved[pair, q, 0], NT) - dot(real, moved[pair, q, 1], NT)).astype(BF16)


def main_kernel(
    count, cuts, rows,
    mom_ref, perm_ref, sign_ref, site_ref, vec_hbm, tau_hbm,
    out_ref, sink_ref,
    phase, vecs, turned, acc, tau, spins, moved, mixed, part, held, whole, table,
    vec_sem, tau_sem, send_sem, recv_sem, back_send, back_recv, sink_send, sink_recv,
):
    time, me = lax.axis_index("ta"), lax.axis_index("gx")
    depth, lanes = vecs.shape[0], vecs.shape[-1]
    chunks = COLOR * cuts

    def fetch(i):
        span = pl.ds(pl.multiple_of(lax.rem(i, cuts) * lanes, lanes), lanes)
        return pltpu.make_async_copy(vec_hbm.at[:, i // cuts, :, span], vecs.at[lax.rem(i, depth)], vec_sem.at[lax.rem(i, depth)])

    for i in range(depth - 1):
        fetch(i).start()
    fetch_tau = pltpu.make_async_copy(tau_hbm, tau, tau_sem)
    fetch_tau.start()

    barrier = pltpu.get_barrier_semaphore()
    for hop in range(1, count):
        pl.semaphore_signal(barrier, inc=1, device_id={"gx": lax.rem(me + hop, count)}, device_id_type=MESH)
    for b in range(2):
        source = 2 * me + b
        holder = lax.rem(time + me - source - 1 + 4 * count, count)
        pl.semaphore_signal(barrier, inc=1, device_id={"ta": source, "gx": holder}, device_id_type=MESH)

    load_phases(mom_ref, site_ref, phase)
    acc[...] = jnp.zeros_like(acc)

    @pl.loop(0, chunks)
    def _(i):
        fetch(i).wait()

        @pl.when(i + depth - 1 < chunks)
        def _():
            fetch(i + depth - 1).start()

        project_chunk(vecs.at[lax.rem(i, depth)], phase, lax.rem(i, cuts), turned, acc, lanes)

    norm = 0.5 / math.sqrt(COLOR * SITES * NEV)
    half = count // 2
    width = PAIR // count
    real = (acc[0:NEV, 0:PAIR] + acc[NEV:PAIR, PAIR:NDIM]) * norm
    imag = (acc[0:NEV, PAIR:NDIM] - acc[NEV:PAIR, 0:PAIR]) * norm
    part[0:half] = real.astype(BF16).reshape(half, width, PAIR)
    part[half:count] = imag.astype(BF16).reshape(half, width, PAIR)

    pl.semaphore_wait(barrier, count + 1)
    copies = []
    for hop in range(1, count):
        peer = lax.rem(me + hop, count)
        copy = pltpu.make_async_remote_copy(
            src_ref=part.at[peer], dst_ref=held.at[hop],
            send_sem=send_sem.at[hop], recv_sem=recv_sem.at[hop],
            device_id={"gx": peer}, device_id_type=MESH,
        )
        copy.start()
        copies.append(copy)
    fetch_tau.wait()
    arrange(0, perm_ref, sign_ref, tau, spins, moved)
    total = part[me].astype(F32)
    for hop in range(1, count):
        copies[hop - 1].wait_recv()
        total = total + held[hop].astype(F32)
    whole[me] = total.astype(BF16)
    backs = []
    for hop in range(1, count):
        back = pltpu.make_async_remote_copy(
            src_ref=whole.at[me], dst_ref=whole.at[me],
            send_sem=back_send.at[hop], recv_sem=back_recv.at[hop],
            device_id={"gx": lax.rem(me + hop, count)}, device_id_type=MESH,
        )
        back.start()
        backs.append(back)
    arrange(1, perm_ref, sign_ref, tau, spins, moved)
    for hop in range(1, count):
        copies[hop - 1].wait_send()
        backs[hop - 1].wait()

    slot = lax.rem(time, 2)
    target = time // 2
    sinks = []
    for h in range(2):
        to = lax.rem(me - target + time + 1 + count, count) + h * count
        sink = pltpu.make_async_remote_copy(
            src_ref=whole, dst_ref=sink_ref.at[slot],
            send_sem=sink_send.at[h], recv_sem=sink_recv.at[slot],
            device_id={"ta": to, "gx": target}, device_id_type=MESH,
        )
        sink.start()
        sinks.append(sink)

    first = whole[0:half].reshape(NEV, PAIR)
    second = whole[half:count].reshape(NEV, PAIR)
    table[0:NEV, 0:PAIR] = first
    table[0:NEV, PAIR:NDIM] = second
    table[NEV:PAIR, 0:PAIR] = -second
    table[NEV:PAIR, PAIR:NDIM] = first

    blocks = NDIM // rows

    @pl.loop(0, 2 * blocks)
    def _(i):
        start = pl.multiple_of(lax.rem(i, blocks) * rows, rows)
        close_rows(i // blocks, start, rows, table, spins, moved, mixed, out_ref)

    for h in range(2):
        sinks[h].wait_send()
    for b in range(2):
        pltpu.make_async_remote_copy(
            src_ref=whole, dst_ref=sink_ref.at[b],
            send_sem=sink_send.at[b], recv_sem=sink_recv.at[b],
            device_id={"gx": lax.rem(me + 1, count)}, device_id_type=MESH,
        ).wait_recv()


def pinned(array):
    return pltpu.with_memory_space_constraint(array, pltpu.HBM)


def main_call(momenta, spin_perm, spin_sign, site_index, vectors, peram, count, chunk=1024, rows=384):
    sites = vectors.shape[-1]
    cuts = sites // chunk
    width = PAIR // count
    smem = pl.BlockSpec(memory_space=pltpu.SMEM)
    vmem = pl.BlockSpec(memory_space=pltpu.VMEM)
    hbm = pl.BlockSpec(memory_space=pltpu.HBM)
    dma = pltpu.SemaphoreType.DMA
    return pl.pallas_call(
        functools.partial(main_kernel, count, cuts, rows),
        out_shape=(
            pltpu.VMEM((2, 2, 2, NDIM, NDIM), BF16),
            pltpu.VMEM((2, count, width, PAIR), BF16),
        ),
        in_specs=[smem, smem, smem, vmem, hbm, hbm],
        out_specs=(vmem, vmem),
        scratch_shapes=[
            pltpu.VMEM((4, cuts, chunk // LANE, LANE), F32),
            pltpu.VMEM((DEPTH, 2, NEV, chunk), BF16),
            pltpu.VMEM((NDIM, chunk), BF16),
            pltpu.VMEM((PAIR, NDIM), F32),
            pltpu.VMEM((2, 2, NDIM, NDIM), BF16),
            pltpu.VMEM((2, SPIN, NDIM, PAIR), BF16),
            pltpu.VMEM((2, 2, 2, NDIM, NDIM), BF16),
            pltpu.VMEM((2, 2, rows, NDIM), BF16),
            pltpu.VMEM((count, width, PAIR), BF16),
            pltpu.VMEM((count, width, PAIR), BF16),
            pltpu.VMEM((count, width, PAIR), BF16),
            pltpu.VMEM((PAIR, NDIM), BF16),
            dma((DEPTH,)),
            dma,
            dma((count,)),
            dma((count,)),
            dma((count,)),
            dma((count,)),
            dma((2,)),
            dma((2,)),
        ],
        compiler_params=pltpu.CompilerParams(
            collective_id=0, has_side_effects=True, vmem_limit_bytes=42 * 1024 * 1024
        ),
        name="project_sum_close",
    )(momenta, spin_perm, spin_sign, site_index.reshape(cuts, chunk // LANE, LANE), pinned(vectors), pinned(peram))


def apply_kernel(perm_ref, sign_ref, elem_ref, x_ref, out0_ref, out1_ref, table):
    pair, r = pl.program_id(0), pl.program_id(1)

    @pl.when(r == 0)
    def _():
        for d in range(2):
            real = elem_ref[pair, 0:NEV, d * NEV : (d + 1) * NEV]
            imag = elem_ref[pair, NEV:PAIR, d * NEV : (d + 1) * NEV]
            table[d, 0:NEV, 0:NEV] = real
            table[d, 0:NEV, NEV:PAIR] = -imag
            table[d, NEV:PAIR, 0:NEV] = imag
            table[d, NEV:PAIR, NEV:PAIR] = real

    chiral = jnp.where(lax.broadcasted_iota(jnp.int32, (1, NDIM), 1) < NDIM // 2, 1.0, -1.0)
    weights = chiral * (0.5 / math.sqrt(NDIM))
    for d, out_ref in ((0, out0_ref), (1, out1_ref)):
        span = pl.ds(pl.multiple_of(perm_ref[d, r] * NEV, NEV), NEV)
        sign = (2 * sign_ref[d, r] - 1).astype(F32)
        stacked = jnp.concatenate([x_ref[1 - d, 0, pair, span, :], x_ref[1 - d, 1, pair, span, :]], axis=0)
        done = dot(table[d], stacked) * (weights * sign)
        out_ref[0, 0, 0] = done[0:NEV].astype(BF16)
        out_ref[1, 0, 0] = done[NEV:PAIR].astype(BF16)


def apply_sinks(elem, blocks, spin_perm, spin_sign, interpret=False):
    sinks = blocks.shape[2]
    shape = jax.ShapeDtypeStruct((2, sinks, 1, NDIM, NDIM), BF16)
    out_spec = pl.BlockSpec((2, 1, 1, NEV, NDIM), lambda i, j: (0, i, 0, j, 0))
    smem = pl.BlockSpec(memory_space=pltpu.SMEM)
    vmem = pl.BlockSpec(memory_space=pltpu.VMEM)
    return pl.pallas_call(
        apply_kernel,
        out_shape=(shape, shape),
        grid=(sinks, SPIN),
        in_specs=[smem, smem, vmem, vmem],
        out_specs=(out_spec, out_spec),
        scratch_shapes=[pltpu.VMEM((2, PAIR, PAIR), BF16)],
        compiler_params=pltpu.CompilerParams(
            dimension_semantics=("arbitrary", "arbitrary"), vmem_limit_bytes=24 * 1024 * 1024
        ),
        name="apply_sinks",
        interpret=interpret,
    )(spin_perm, spin_sign, elem, blocks)


def on_device(count, eigenvectors, site_index, momenta, perambulators, spin_perm, spin_sign):
    vectors = jnp.transpose(eigenvectors[0], (0, 2, 3, 1))
    blocks, elem = main_call(
        momenta, spin_perm, spin_sign, site_index, vectors, perambulators[:, :, 0], count
    )
    return apply_sinks(elem.reshape(2, PAIR, PAIR), blocks, spin_perm, spin_sign)


def solution(mesh):
    return jax.shard_map(
        functools.partial(on_device, mesh.shape["gx"]),
        mesh=mesh,
        in_specs=(
            P("ta", None, "gx", None, None),
            P("gx"),
            P(),
            P(None, "gx", "ta", None, None),
            P(),
            P(),
        ),
        out_specs=(P(None, "gx", "ta", None, None), P(None, "gx", "ta", None, None)),
        check_vma=False,
    )
```

```python
import functools
import math

import jax
import jax.numpy as jnp
from jax import lax
from jax.experimental import pallas as pl
from jax.experimental.pallas import tpu as pltpu
from jax.sharding import PartitionSpec as P

L = 32
NEV = 192
COLOR = 3
SPIN = 4
SITES = 32768
NDIM = SPIN * NEV
PAIR = 2 * NEV
LANE = 128
DEPTH = 4
MESH = pl.DeviceIdType.MESH
F32 = jnp.float32
BF16 = jnp.bfloat16
NT = (((1,), (1,)), ((), ()))
NN = (((1,), (0,)), ((), ()))


def dot(a, b, dims=NN):
    return lax.dot_general(a, b, dims, preferred_element_type=F32)


FIRST = (3, 5, 6, 0, 2, 4, 7, 1)
TWIST = (0, 2, 6, 4, 5, 7, 3, 1)
SOURCE = [[a ^ b for a in FIRST] for b in TWIST]
TARGET = [[row.index(chip) for chip in range(8)] for row in SOURCE]


def look_up(table, i, j):
    found = 0
    for a, row in enumerate(table):
        for b, value in enumerate(row):
            found = found + jnp.where((i == a) & (j == b), value, 0)
    return found


def load_phases(mom_ref, site_ref, phase):
    site = site_ref[...]
    first, second, third = site >> 10, (site >> 5) & (L - 1), site & (L - 1)
    for p in range(2):
        dotted = mom_ref[p, 0] * first + mom_ref[p, 1] * second + mom_ref[p, 2] * third
        angle = (dotted & (L - 1)).astype(F32) * (2.0 * math.pi / L)
        phase[2 * p] = jnp.cos(angle)
        phase[2 * p + 1] = jnp.sin(angle)


def turn_chunk(vec, phase, cut, turned, lanes):
    for j in range(lanes // LANE):
        span = slice(j * LANE, (j + 1) * LANE)
        real = vec[0, :, span].astype(F32)
        imag = vec[1, :, span].astype(F32)
        for p in range(2):
            cosine = phase[2 * p, cut, j : j + 1, :]
            sine = phase[2 * p + 1, cut, j : j + 1, :]
            turned[p * NEV : (p + 1) * NEV, span] = (cosine * real - sine * imag).astype(BF16)
            turned[PAIR + p * NEV : PAIR + (p + 1) * NEV, span] = (cosine * imag + sine * real).astype(BF16)


def arrange(pair, perm_ref, sign_ref, tau, spins, moved):
    for a in range(SPIN):
        cut = slice(a * NEV, (a + 1) * NEV)
        spins[pair, a, :, 0:NEV] = tau[0, pair, :, cut]
        spins[pair, a, :, NEV:PAIR] = tau[1, pair, :, cut]
    for q in range(2):
        for a in range(SPIN):
            into = perm_ref[q, a]
            sign = (2 * sign_ref[q, a] - 1) * jnp.where(into < SPIN // 2, 1, -1)
            block = spins[pair, into] * sign.astype(F32).astype(BF16)
            moved[pair, q, 0, :, a * NEV : (a + 1) * NEV] = block[:, 0:NEV]
            moved[pair, q, 1, :, a * NEV : (a + 1) * NEV] = block[:, NEV:PAIR]


def close_rows(pair, start, rows, table, spins, moved, mixed, out_ref):
    for a in range(SPIN):
        product = dot(spins[pair, a, pl.ds(start, rows), :], table[...]).astype(BF16)
        for c in range(2):
            for q in range(2):
                left = c * PAIR + q * NEV
                mixed[q, c, :, a * NEV : (a + 1) * NEV] = product[:, left : left + NEV]
    for q in range(2):
        real, imag = mixed[q, 0], mixed[q, 1]
        keep = pl.ds(start, rows)
        out_ref[q, 0, pair, keep, :] = (dot(real, moved[pair, q, 0], NT) + dot(imag, moved[pair, q, 1], NT)).astype(BF16)
        out_ref[q, 1, pair, keep, :] = (dot(imag, moved[pair, q, 0], NT) - dot(real, moved[pair, q, 1], NT)).astype(BF16)


def main_kernel(
    count, cuts, rows,
    mom_hbm, perm_hbm, sign_hbm, site_hbm, vec_hbm, tau_hbm,
    out_ref, sink_ref,
    mom_ref, perm_ref, sign_ref, site_ref, phase, vecs, even, odd, acc, tau, spins, moved, mixed, part, held, whole, table,
    small_sem, vec_sem, tau_sem, send_sem, recv_sem, back_send, back_recv, sink_send, sink_recv,
):
    time, me = lax.axis_index("ta"), lax.axis_index("gx")
    depth, lanes = vecs.shape[0], vecs.shape[-1]
    chunks = COLOR * cuts
    small = ((mom_hbm, mom_ref), (site_hbm, site_ref), (perm_hbm, perm_ref), (sign_hbm, sign_ref))
    small = [pltpu.make_async_copy(a, b, small_sem.at[k]) for k, (a, b) in enumerate(small)]

    def fetch(i):
        source = vec_hbm.at[:, i // cuts, :, i % cuts * lanes : (i % cuts + 1) * lanes]
        return pltpu.make_async_copy(source, vecs.at[i % depth], vec_sem.at[i % depth])

    for copy in small:
        copy.start()
    for i in range(depth):
        fetch(i).start()
    fetch_tau = pltpu.make_async_copy(tau_hbm, tau, tau_sem)
    fetch_tau.start()

    slot = lax.rem(time, 2)
    sibling = {"ta": time + 1 - 2 * slot}
    barrier = pltpu.get_barrier_semaphore()
    for hop in range(1, count):
        pl.semaphore_signal(barrier, inc=1, device_id={"gx": lax.rem(me + hop, count)}, device_id_type=MESH)
    source = {"ta": 2 * me + slot, "gx": look_up(SOURCE, me, time // 2)}
    pl.semaphore_signal(barrier, inc=1, device_id=source, device_id_type=MESH)
    pl.semaphore_signal(barrier, inc=1, device_id=sibling, device_id_type=MESH)

    small[0].wait()
    small[1].wait()
    load_phases(mom_ref, site_ref, phase)
    fetch(0).wait()
    turn_chunk(vecs.at[0], phase, 0, even, lanes)
    for i in range(chunks):
        if i + 1 < chunks:
            fetch(i + 1).wait()
            turn_chunk(vecs.at[(i + 1) % depth], phase, (i + 1) % cuts, even if i % 2 else odd, lanes)
        plain = jnp.concatenate([vecs[i % depth, 0], vecs[i % depth, 1]], axis=0)
        product = dot(plain, (odd if i % 2 else even)[...], NT)
        acc[...] = product if i == 0 else acc[...] + product
        if i + depth < chunks:
            fetch(i + depth).start()
    small[2].wait()
    small[3].wait()

    norm = 0.5 / math.sqrt(COLOR * SITES * NEV)
    half = count // 2
    width = PAIR // count
    real = (acc[0:NEV, 0:PAIR] + acc[NEV:PAIR, PAIR:NDIM]) * norm
    imag = (acc[0:NEV, PAIR:NDIM] - acc[NEV:PAIR, 0:PAIR]) * norm
    part[0:half] = real.astype(BF16).reshape(half, width, PAIR)
    part[half:count] = imag.astype(BF16).reshape(half, width, PAIR)

    pl.semaphore_wait(barrier, count + 1)
    copies = []
    for hop in range(1, count):
        peer = lax.rem(me + hop, count)
        copy = pltpu.make_async_remote_copy(
            src_ref=part.at[peer], dst_ref=held.at[hop],
            send_sem=send_sem.at[hop], recv_sem=recv_sem.at[hop],
            device_id={"gx": peer}, device_id_type=MESH,
        )
        copy.start()
        copies.append(copy)
    fetch_tau.wait()
    arrange(0, perm_ref, sign_ref, tau, spins, moved)
    total = part[me].astype(F32)
    for hop in range(1, count):
        copies[hop - 1].wait_recv()
        total = total + held[hop].astype(F32)
    whole[me] = total.astype(BF16)
    backs = []
    for hop in range(1, count):
        back = pltpu.make_async_remote_copy(
            src_ref=whole.at[me], dst_ref=whole.at[me],
            send_sem=back_send.at[hop], recv_sem=back_recv.at[hop],
            device_id={"gx": lax.rem(me + hop, count)}, device_id_type=MESH,
        )
        back.start()
        backs.append(back)
    arrange(1, perm_ref, sign_ref, tau, spins, moved)
    for hop in range(1, count):
        copies[hop - 1].wait_send()
        backs[hop - 1].wait()

    target = time // 2
    sink = pltpu.make_async_remote_copy(
        src_ref=whole, dst_ref=sink_ref.at[slot], send_sem=sink_send.at[0], recv_sem=sink_recv.at[0],
        device_id={"ta": 2 * look_up(TARGET, target, me) + slot, "gx": target}, device_id_type=MESH,
    )
    sink.start()

    first = whole[0:half].reshape(NEV, PAIR)
    second = whole[half:count].reshape(NEV, PAIR)
    table[0:NEV, 0:PAIR] = first
    table[0:NEV, PAIR:NDIM] = second
    table[NEV:PAIR, 0:PAIR] = -second
    table[NEV:PAIR, PAIR:NDIM] = first

    blocks = NDIM // rows
    last = 2 * blocks - 1
    onward = pltpu.make_async_remote_copy(
        src_ref=sink_ref.at[slot], dst_ref=sink_ref.at[slot], send_sem=sink_send.at[1], recv_sem=sink_recv.at[1],
        device_id=sibling, device_id_type=MESH,
    )

    @pl.loop(0, last + 1)
    def _(i):
        @pl.when(i == last)
        def _():
            sink.wait_recv()
            onward.start()

        start = pl.multiple_of(lax.rem(i, blocks) * rows, rows)
        close_rows(i // blocks, start, rows, table, spins, moved, mixed, out_ref)

    sink.wait_send()
    onward.wait()


def pinned(array):
    return pltpu.with_memory_space_constraint(array, pltpu.HBM)


def main_call(momenta, spin_perm, spin_sign, site_index, vectors, peram, count, chunk=1024, rows=384):
    sites = vectors.shape[-1]
    cuts = sites // chunk
    width = PAIR // count
    vmem = pl.BlockSpec(memory_space=pltpu.VMEM)
    hbm = pl.BlockSpec(memory_space=pltpu.HBM)
    dma = pltpu.SemaphoreType.DMA
    return pl.pallas_call(
        functools.partial(main_kernel, count, cuts, rows),
        out_shape=(
            pltpu.VMEM((2, 2, 2, NDIM, NDIM), BF16),
            pltpu.VMEM((2, count, width, PAIR), BF16),
        ),
        in_specs=[hbm] * 6,
        out_specs=(vmem, vmem),
        scratch_shapes=[
            pltpu.SMEM(momenta.shape, jnp.int32),
            pltpu.SMEM(spin_perm.shape, jnp.int32),
            pltpu.SMEM(spin_sign.shape, jnp.int32),
            pltpu.VMEM((cuts, chunk // LANE, LANE), jnp.int32),
            pltpu.VMEM((4, cuts, chunk // LANE, LANE), F32),
            pltpu.VMEM((DEPTH, 2, NEV, chunk), BF16),
            pltpu.VMEM((NDIM, chunk), BF16),
            pltpu.VMEM((NDIM, chunk), BF16),
            pltpu.VMEM((PAIR, NDIM), F32),
            pltpu.VMEM((2, 2, NDIM, NDIM), BF16),
            pltpu.VMEM((2, SPIN, NDIM, PAIR), BF16),
            pltpu.VMEM((2, 2, 2, NDIM, NDIM), BF16),
            pltpu.VMEM((2, 2, rows, NDIM), BF16),
            pltpu.VMEM((count, width, PAIR), BF16),
            pltpu.VMEM((count, width, PAIR), BF16),
            pltpu.VMEM((count, width, PAIR), BF16),
            pltpu.VMEM((PAIR, NDIM), BF16),
            dma((4,)),
            dma((DEPTH,)),
            dma,
            dma((count,)),
            dma((count,)),
            dma((count,)),
            dma((count,)),
            dma((2,)),
            dma((2,)),
        ],
        compiler_params=pltpu.CompilerParams(
            collective_id=0, has_side_effects=True, vmem_limit_bytes=42 * 1024 * 1024
        ),
        name="project_sum_close",
    )(*map(pinned, (momenta, spin_perm, spin_sign, site_index.reshape(cuts, chunk // LANE, LANE), vectors, peram)))


def apply_kernel(perm_ref, sign_ref, elem_ref, x_ref, out0_ref, out1_ref, table):
    pair, r = pl.program_id(0), pl.program_id(1)

    @pl.when(r == 0)
    def _():
        for d in range(2):
            real = elem_ref[pair, 0:NEV, d * NEV : (d + 1) * NEV]
            imag = elem_ref[pair, NEV:PAIR, d * NEV : (d + 1) * NEV]
            table[d, 0:NEV, 0:NEV] = real
            table[d, 0:NEV, NEV:PAIR] = -imag
            table[d, NEV:PAIR, 0:NEV] = imag
            table[d, NEV:PAIR, NEV:PAIR] = real

    chiral = jnp.where(lax.broadcasted_iota(jnp.int32, (1, NDIM), 1) < NDIM // 2, 1.0, -1.0)
    weights = chiral * (0.5 / math.sqrt(NDIM))
    for d, out_ref in ((0, out0_ref), (1, out1_ref)):
        span = pl.ds(pl.multiple_of(perm_ref[d, r] * NEV, NEV), NEV)
        sign = (2 * sign_ref[d, r] - 1).astype(F32)
        stacked = jnp.concatenate([x_ref[1 - d, 0, pair, span, :], x_ref[1 - d, 1, pair, span, :]], axis=0)
        done = dot(table[d], stacked) * (weights * sign)
        out_ref[0, 0, 0] = done[0:NEV].astype(BF16)
        out_ref[1, 0, 0] = done[NEV:PAIR].astype(BF16)


def apply_sinks(elem, blocks, spin_perm, spin_sign, interpret=False):
    sinks = blocks.shape[2]
    shape = jax.ShapeDtypeStruct((2, sinks, 1, NDIM, NDIM), BF16)
    out_spec = pl.BlockSpec((2, 1, 1, NEV, NDIM), lambda i, j: (0, i, 0, j, 0))
    smem = pl.BlockSpec(memory_space=pltpu.SMEM)
    vmem = pl.BlockSpec(memory_space=pltpu.VMEM)
    return pl.pallas_call(
        apply_kernel,
        out_shape=(shape, shape),
        grid=(sinks, SPIN),
        in_specs=[smem, smem, vmem, vmem],
        out_specs=(out_spec, out_spec),
        scratch_shapes=[pltpu.VMEM((2, PAIR, PAIR), BF16)],
        compiler_params=pltpu.CompilerParams(
            dimension_semantics=("arbitrary", "arbitrary"), vmem_limit_bytes=24 * 1024 * 1024
        ),
        name="apply_sinks",
        interpret=interpret,
    )(spin_perm, spin_sign, elem, blocks)


def on_device(count, eigenvectors, site_index, momenta, perambulators, spin_perm, spin_sign):
    vectors = jnp.transpose(eigenvectors[0], (0, 2, 3, 1))
    blocks, elem = main_call(
        momenta, spin_perm, spin_sign, site_index, vectors, perambulators[:, :, 0], count
    )
    return apply_sinks(elem.reshape(2, PAIR, PAIR), blocks, spin_perm, spin_sign)


def solution(mesh):
    return jax.shard_map(
        functools.partial(on_device, mesh.shape["gx"]),
        mesh=mesh,
        in_specs=(
            P("ta", None, "gx", None, None),
            P("gx"),
            P(),
            P(None, "gx", "ta", None, None),
            P(),
            P(),
        ),
        out_specs=(P(None, "gx", "ta", None, None), P(None, "gx", "ta", None, None)),
        check_vma=False,
    )
```

```python
import functools
import math

import jax
import jax.numpy as jnp
from jax import lax
from jax.experimental import pallas as pl
from jax.experimental.pallas import tpu as pltpu
from jax.sharding import PartitionSpec as P

L = 32
NEV = 192
COLOR = 3
SPIN = 4
SITES = 32768
NDIM = SPIN * NEV
PAIR = 2 * NEV
LANE = 128
DEPTH = 3
MESH = pl.DeviceIdType.MESH
F32 = jnp.float32
BF16 = jnp.bfloat16
NT = (((1,), (1,)), ((), ()))
NN = (((1,), (0,)), ((), ()))


def dot(a, b, dims=NN):
    return lax.dot_general(a, b, dims, preferred_element_type=F32)


FIRST = (3, 5, 6, 0, 2, 4, 7, 1)
TWIST = (0, 2, 6, 4, 5, 7, 3, 1)
SOURCE = [[a ^ b for a in FIRST] for b in TWIST]
TARGET = [[row.index(chip) for chip in range(8)] for row in SOURCE]


def look_up(table, i, j):
    found = 0
    for a, row in enumerate(table):
        for b, value in enumerate(row):
            found = found + jnp.where((i == a) & (j == b), value, 0)
    return found


def load_phases(mom_ref, site_ref, phase):
    site = site_ref[...]
    first, second, third = site >> 10, (site >> 5) & (L - 1), site & (L - 1)
    for p in range(2):
        dotted = mom_ref[p, 0] * first + mom_ref[p, 1] * second + mom_ref[p, 2] * third
        angle = (dotted & (L - 1)).astype(F32) * (2.0 * math.pi / L)
        for k, value in enumerate((jnp.cos(angle), jnp.sin(angle))):
            phase[2 * p + k] = jnp.broadcast_to(value[:, :, None, :], value.shape[:2] + (8, LANE))


def turn_chunk(vec, phase, cut, turned, lanes):
    for j in range(lanes // LANE):
        span = slice(j * LANE, (j + 1) * LANE)
        real = vec[0, :, span].astype(F32).reshape(NEV // 8, 8, LANE)
        imag = vec[1, :, span].astype(F32).reshape(NEV // 8, 8, LANE)
        for p in range(2):
            cosine = phase[2 * p, cut, j][None]
            sine = phase[2 * p + 1, cut, j][None]
            first = (cosine * real - sine * imag).reshape(NEV, LANE)
            second = (cosine * imag + sine * real).reshape(NEV, LANE)
            turned[p * NEV : (p + 1) * NEV, span] = first.astype(BF16)
            turned[PAIR + p * NEV : PAIR + (p + 1) * NEV, span] = second.astype(BF16)


def arrange(pair, perm_ref, sign_ref, tau, spins, moved, rows=128):
    @pl.loop(0, NDIM // rows)
    def _(i):
        keep = pl.ds(pl.multiple_of(i * rows, rows), rows)
        for a in range(SPIN):
            cut = slice(a * NEV, (a + 1) * NEV)
            spins[pair, a, keep, 0:NEV] = tau[0, pair, keep, cut]
            spins[pair, a, keep, NEV:PAIR] = tau[1, pair, keep, cut]
        for q in range(2):
            for a in range(SPIN):
                into = perm_ref[q, a]
                sign = (2 * sign_ref[q, a] - 1) * jnp.where(into < SPIN // 2, 1, -1)
                block = spins[pair, into, keep, :] * sign.astype(F32).astype(BF16)
                moved[pair, q, 0, keep, a * NEV : (a + 1) * NEV] = block[:, 0:NEV]
                moved[pair, q, 1, keep, a * NEV : (a + 1) * NEV] = block[:, NEV:PAIR]
            real, imag = moved[pair, q, 0, keep, :], moved[pair, q, 1, keep, :]
            moved[pair, q, 2, keep, :] = (real.astype(F32) - imag.astype(F32)).astype(BF16)


def close_rows(pair, start, rows, table, spins, moved, mixed, out_ref, before):
    for a in range(SPIN):
        product = dot(spins[pair, a, pl.ds(start, rows), :], table[...])
        real, imag = product[:, 0:PAIR], product[:, PAIR:NDIM]
        for c, value in enumerate((real, imag, real + imag)):
            value = value.astype(BF16)
            for q in range(2):
                mixed[q, c, :, a * NEV : (a + 1) * NEV] = value[:, q * NEV : (q + 1) * NEV]
    keep = pl.ds(start, rows)

    @pl.loop(0, 2)
    def _(q):
        before(q)
        first = dot(mixed[q, 0], moved[pair, q, 0], NT)
        second = dot(mixed[q, 1], moved[pair, q, 1], NT)
        third = dot(mixed[q, 2], moved[pair, q, 2], NT)
        out_ref[q, 0, pair, keep, :] = (first + second).astype(BF16)
        out_ref[q, 1, pair, keep, :] = (third - first + second).astype(BF16)


def main_kernel(
    count, cuts, rows,
    mom_hbm, perm_hbm, sign_hbm, site_hbm, vec_hbm, tau_hbm,
    out_ref, sink_ref,
    mom_ref, perm_ref, sign_ref, site_ref, phase, vecs, turned, acc, tau, spins, moved, mixed, part, held, whole, table,
    small_sem, vec_sem, tau_sem, send_sem, recv_sem, back_send, back_recv, sink_send, sink_recv,
):
    time, me = lax.axis_index("ta"), lax.axis_index("gx")
    depth, lanes = vecs.shape[0], vecs.shape[-1]
    chunks = COLOR * cuts
    small = ((mom_hbm, mom_ref), (site_hbm, site_ref), (perm_hbm, perm_ref), (sign_hbm, sign_ref))
    small = [pltpu.make_async_copy(a, b, small_sem.at[k]) for k, (a, b) in enumerate(small)]

    def fetch(i):
        span = pl.ds(pl.multiple_of(lax.rem(i, cuts) * lanes, lanes), lanes)
        turn = lax.rem(i, depth)
        return pltpu.make_async_copy(vec_hbm.at[:, i // cuts, :, span], vecs.at[turn], vec_sem.at[turn])

    for copy in small:
        copy.start()
    for i in range(depth):
        fetch(i).start()
    fetch_tau = pltpu.make_async_copy(tau_hbm, tau, tau_sem)
    fetch_tau.start()

    slot = lax.rem(time, 2)
    sibling = {"ta": time + 1 - 2 * slot}
    barrier = pltpu.get_barrier_semaphore()
    for hop in range(1, count):
        pl.semaphore_signal(barrier, inc=1, device_id={"gx": lax.rem(me + hop, count)}, device_id_type=MESH)
    source = {"ta": 2 * me + slot, "gx": look_up(SOURCE, me, time // 2)}
    pl.semaphore_signal(barrier, inc=1, device_id=source, device_id_type=MESH)
    pl.semaphore_signal(barrier, inc=1, device_id=sibling, device_id_type=MESH)

    small[0].wait()
    small[1].wait()
    load_phases(mom_ref, site_ref, phase)
    fetch(0).wait()
    acc[...] = jnp.zeros_like(acc)

    @pl.loop(0, chunks)
    def _(i):
        @pl.when(i > 0)
        def _():
            fetch(i).wait()

        own = vecs.at[lax.rem(i, depth)]
        turn_chunk(own, phase, lax.rem(i, cuts), turned, lanes)
        plain = jnp.concatenate([own[0], own[1]], axis=0)
        acc[...] += dot(plain, turned[...], NT)

        @pl.when(i + depth < chunks)
        def _():
            fetch(i + depth).start()

    small[2].wait()
    small[3].wait()

    norm = 0.5 / math.sqrt(COLOR * SITES * NEV)
    half = count // 2
    width = PAIR // count
    real = (acc[0:NEV, 0:PAIR] + acc[NEV:PAIR, PAIR:NDIM]) * norm
    imag = (acc[0:NEV, PAIR:NDIM] - acc[NEV:PAIR, 0:PAIR]) * norm
    part[0:half] = real.astype(BF16).reshape(half, width, PAIR)
    part[half:count] = imag.astype(BF16).reshape(half, width, PAIR)

    pl.semaphore_wait(barrier, count + 1)
    copies = []
    for hop in range(1, count):
        peer = lax.rem(me + hop, count)
        copy = pltpu.make_async_remote_copy(
            src_ref=part.at[peer], dst_ref=held.at[hop],
            send_sem=send_sem.at[hop], recv_sem=recv_sem.at[hop],
            device_id={"gx": peer}, device_id_type=MESH,
        )
        copy.start()
        copies.append(copy)
    fetch_tau.wait()
    arrange(0, perm_ref, sign_ref, tau, spins, moved)
    total = part[me].astype(F32)
    for hop in range(1, count):
        copies[hop - 1].wait_recv()
        total = total + held[hop].astype(F32)
    whole[me] = total.astype(BF16)
    backs = []
    for hop in range(1, count):
        back = pltpu.make_async_remote_copy(
            src_ref=whole.at[me], dst_ref=whole.at[me],
            send_sem=back_send.at[hop], recv_sem=back_recv.at[hop],
            device_id={"gx": lax.rem(me + hop, count)}, device_id_type=MESH,
        )
        back.start()
        backs.append(back)
    arrange(1, perm_ref, sign_ref, tau, spins, moved)
    for hop in range(1, count):
        copies[hop - 1].wait_send()
        backs[hop - 1].wait()

    target = time // 2
    sink = pltpu.make_async_remote_copy(
        src_ref=whole, dst_ref=sink_ref.at[slot], send_sem=sink_send.at[0], recv_sem=sink_recv.at[0],
        device_id={"ta": 2 * look_up(TARGET, target, me) + slot, "gx": target}, device_id_type=MESH,
    )
    sink.start()

    first = whole[0:half].reshape(NEV, PAIR)
    second = whole[half:count].reshape(NEV, PAIR)
    table[0:NEV, 0:PAIR] = first
    table[0:NEV, PAIR:NDIM] = second
    table[NEV:PAIR, 0:PAIR] = -second
    table[NEV:PAIR, PAIR:NDIM] = first

    blocks = NDIM // rows
    last = 2 * blocks - 1
    onward = pltpu.make_async_remote_copy(
        src_ref=sink_ref.at[slot], dst_ref=sink_ref.at[slot], send_sem=sink_send.at[1], recv_sem=sink_recv.at[1],
        device_id=sibling, device_id_type=MESH,
    )

    @pl.loop(0, last + 1)
    def _(i):
        def before(q):
            @pl.when((i == last) & (q == 1))
            def _():
                sink.wait_recv()
                onward.start()

        start = pl.multiple_of(lax.rem(i, blocks) * rows, rows)
        close_rows(i // blocks, start, rows, table, spins, moved, mixed, out_ref, before)

    sink.wait_send()
    onward.wait()


def pinned(array):
    return pltpu.with_memory_space_constraint(array, pltpu.HBM)


def main_call(momenta, spin_perm, spin_sign, site_index, vectors, peram, count, chunk=2048, rows=384):
    sites = vectors.shape[-1]
    cuts = sites // chunk
    width = PAIR // count
    vmem = pl.BlockSpec(memory_space=pltpu.VMEM)
    hbm = pl.BlockSpec(memory_space=pltpu.HBM)
    dma = pltpu.SemaphoreType.DMA
    return pl.pallas_call(
        functools.partial(main_kernel, count, cuts, rows),
        out_shape=(
            pltpu.VMEM((2, 2, 2, NDIM, NDIM), BF16),
            pltpu.VMEM((2, count, width, PAIR), BF16),
        ),
        in_specs=[hbm] * 6,
        out_specs=(vmem, vmem),
        scratch_shapes=[
            pltpu.SMEM(momenta.shape, jnp.int32),
            pltpu.SMEM(spin_perm.shape, jnp.int32),
            pltpu.SMEM(spin_sign.shape, jnp.int32),
            pltpu.VMEM((cuts, chunk // LANE, LANE), jnp.int32),
            pltpu.VMEM((4, cuts, chunk // LANE, 8, LANE), F32),
            pltpu.VMEM((DEPTH, 2, NEV, chunk), BF16),
            pltpu.VMEM((NDIM, chunk), BF16),
            pltpu.VMEM((PAIR, NDIM), F32),
            pltpu.VMEM((2, 2, NDIM, NDIM), BF16),
            pltpu.VMEM((2, SPIN, NDIM, PAIR), BF16),
            pltpu.VMEM((2, 2, 3, NDIM, NDIM), BF16),
            pltpu.VMEM((2, 3, rows, NDIM), BF16),
            pltpu.VMEM((count, width, PAIR), BF16),
            pltpu.VMEM((count, width, PAIR), BF16),
            pltpu.VMEM((count, width, PAIR), BF16),
            pltpu.VMEM((PAIR, NDIM), BF16),
            dma((4,)),
            dma((DEPTH,)),
            dma,
            dma((count,)),
            dma((count,)),
            dma((count,)),
            dma((count,)),
            dma((2,)),
            dma((2,)),
        ],
        compiler_params=pltpu.CompilerParams(
            collective_id=0, has_side_effects=True, vmem_limit_bytes=48 * 1024 * 1024
        ),
        name="project_sum_close",
    )(*map(pinned, (momenta, spin_perm, spin_sign, site_index.reshape(cuts, chunk // LANE, LANE), vectors, peram)))


def apply_kernel(group, perm_hbm, sign_hbm, elem_ref, x_ref, out0_hbm, out1_hbm, perm_ref, sign_ref, table, stage, small_sem, out_sem):
    sinks = x_ref.shape[2]
    parts = SPIN // group
    small = [
        pltpu.make_async_copy(perm_hbm, perm_ref, small_sem.at[0]),
        pltpu.make_async_copy(sign_hbm, sign_ref, small_sem.at[1]),
    ]
    for copy in small:
        copy.start()

    @pl.loop(0, 2 * sinks)
    def _(n):
        pair, d = n // 2, lax.rem(n, 2)
        both_real, both_imag = elem_ref[pair, 0:NEV], elem_ref[pair, NEV:PAIR]
        real = jnp.where(d == 0, both_real[:, 0:NEV], both_real[:, NEV:PAIR])
        imag = jnp.where(d == 0, both_imag[:, 0:NEV], both_imag[:, NEV:PAIR])
        table[n, 0:NEV, 0:NEV] = real
        table[n, 0:NEV, NEV:PAIR] = -imag
        table[n, NEV:PAIR, 0:NEV] = imag
        table[n, NEV:PAIR, NEV:PAIR] = real

    for copy in small:
        copy.wait()
    chiral = jnp.where(lax.broadcasted_iota(jnp.int32, (1, NDIM), 1) < NDIM // 2, 1.0, -1.0)
    weights = chiral * (0.5 / math.sqrt(NDIM))
    steps = sinks * 2 * parts

    def where(i):
        n, part = i // parts, lax.rem(i, parts)
        return n, n // 2, lax.rem(n, 2), part, lax.rem(i, 2)

    def store(i, out_hbm):
        n, pair, d, part, slot = where(i)
        keep = pl.ds(pl.multiple_of(part * group * NEV, group * NEV), group * NEV)
        return pltpu.make_async_copy(stage.at[slot], out_hbm.at[:, pair, 0, keep, :], out_sem.at[slot])

    @pl.loop(0, steps)
    def _(i):
        n, pair, d, part, slot = where(i)

        @pl.when(i >= 2)
        def _():
            store(i, out0_hbm).wait()

        wide = []
        for r in range(group):
            span = pl.ds(pl.multiple_of(perm_ref[d, part * group + r] * NEV, NEV), NEV)
            wide.append(jnp.concatenate([x_ref[1 - d, 0, pair, span, :], x_ref[1 - d, 1, pair, span, :]], axis=0))
        done = dot(table[n], jnp.concatenate(wide, axis=1))
        for r in range(group):
            sign = (2 * sign_ref[d, part * group + r] - 1).astype(F32)
            block = done[:, r * NDIM : (r + 1) * NDIM] * (weights * sign)
            stage[slot, 0, r * NEV : (r + 1) * NEV] = block[0:NEV].astype(BF16)
            stage[slot, 1, r * NEV : (r + 1) * NEV] = block[NEV:PAIR].astype(BF16)

        @pl.when(d == 0)
        def _():
            store(i, out0_hbm).start()

        @pl.when(d == 1)
        def _():
            store(i, out1_hbm).start()

    for i in (steps - 2, steps - 1):
        store(i, out0_hbm).wait()


def apply_sinks(elem, blocks, spin_perm, spin_sign, group=4, interpret=False):
    sinks = blocks.shape[2]
    shape = jax.ShapeDtypeStruct((2, sinks, 1, NDIM, NDIM), BF16)
    vmem = pl.BlockSpec(memory_space=pltpu.VMEM)
    hbm = pl.BlockSpec(memory_space=pltpu.HBM)
    return pl.pallas_call(
        functools.partial(apply_kernel, group),
        out_shape=(shape, shape),
        in_specs=[hbm, hbm, vmem, vmem],
        out_specs=(hbm, hbm),
        scratch_shapes=[
            pltpu.SMEM(spin_perm.shape, jnp.int32),
            pltpu.SMEM(spin_sign.shape, jnp.int32),
            pltpu.VMEM((2 * sinks, PAIR, PAIR), BF16),
            pltpu.VMEM((2, 2, group * NEV, NDIM), BF16),
            pltpu.SemaphoreType.DMA((2,)),
            pltpu.SemaphoreType.DMA((2,)),
        ],
        compiler_params=pltpu.CompilerParams(vmem_limit_bytes=24 * 1024 * 1024),
        name="apply_sinks",
        interpret=interpret,
    )(pinned(spin_perm), pinned(spin_sign), elem, blocks)


def on_device(count, eigenvectors, site_index, momenta, perambulators, spin_perm, spin_sign):
    vectors = jnp.transpose(eigenvectors[0], (0, 2, 3, 1))
    blocks, elem = main_call(
        momenta, spin_perm, spin_sign, site_index, vectors, perambulators[:, :, 0], count
    )
    return apply_sinks(elem.reshape(2, PAIR, PAIR), blocks, spin_perm, spin_sign)


def solution(mesh):
    return jax.shard_map(
        functools.partial(on_device, mesh.shape["gx"]),
        mesh=mesh,
        in_specs=(
            P("ta", None, "gx", None, None),
            P("gx"),
            P(),
            P(None, "gx", "ta", None, None),
            P(),
            P(),
        ),
        out_specs=(P(None, "gx", "ta", None, None), P(None, "gx", "ta", None, None)),
        check_vma=False,
    )
```

```python
import functools
import math

import jax
import jax.numpy as jnp
from jax import lax
from jax.experimental import pallas as pl
from jax.experimental.pallas import tpu as pltpu
from jax.sharding import PartitionSpec as P

L = 32
NEV = 192
COLOR = 3
SPIN = 4
SITES = 32768
NDIM = SPIN * NEV
PAIR = 2 * NEV
LANE = 128
WIDTH = 256
DEPTH = 3
MESH = pl.DeviceIdType.MESH
F32 = jnp.float32
BF16 = jnp.bfloat16
NT = (((1,), (1,)), ((), ()))
NN = (((1,), (0,)), ((), ()))


def dot(a, b, dims=NN):
    return lax.dot_general(a, b, dims, preferred_element_type=F32)


FIRST = (3, 5, 6, 0, 2, 4, 7, 1)
TWIST = (0, 2, 6, 4, 5, 7, 3, 1)
SOURCE = [[a ^ b for a in FIRST] for b in TWIST]
TARGET = [[row.index(chip) for chip in range(8)] for row in SOURCE]


def look_up(table, i, j):
    found = 0
    for a, row in enumerate(table):
        for b, value in enumerate(row):
            found = found + jnp.where((i == a) & (j == b), value, 0)
    return found


def load_phases(mom_ref, site_ref, phase):
    site = site_ref[...]
    first, second, third = site >> 10, (site >> 5) & (L - 1), site & (L - 1)
    for p in range(2):
        dotted = mom_ref[p, 0] * first + mom_ref[p, 1] * second + mom_ref[p, 2] * third
        angle = (dotted & (L - 1)).astype(F32) * (2.0 * math.pi / L)
        for k, value in enumerate((jnp.cos(angle), jnp.sin(angle))):
            phase[2 * p + k] = jnp.broadcast_to(value[:, :, None, :], value.shape[:2] + (8, LANE))


def turn_chunk(vec, phase, cut, turned, lanes):
    for j in range(lanes // LANE):
        span = slice(j * LANE, (j + 1) * LANE)
        real = vec[0, :, span].astype(F32).reshape(NEV // 8, 8, LANE)
        imag = vec[1, :, span].astype(F32).reshape(NEV // 8, 8, LANE)
        for p in range(2):
            cosine = phase[2 * p, cut, j][None]
            sine = phase[2 * p + 1, cut, j][None]
            first = (cosine * real - sine * imag).reshape(NEV, LANE)
            second = (cosine * imag + sine * real).reshape(NEV, LANE)
            turned[p * NEV : (p + 1) * NEV, span] = first.astype(BF16)
            turned[PAIR + p * NEV : PAIR + (p + 1) * NEV, span] = second.astype(BF16)


def arrange(pair, perm_ref, sign_ref, tau, spins, moved, rows=128):
    @pl.loop(0, NDIM // rows)
    def _(i):
        keep = pl.ds(pl.multiple_of(i * rows, rows), rows)
        for a in range(SPIN):
            cut = slice(a * NEV, (a + 1) * NEV)
            spins[pair, a, keep, 0:NEV] = tau[0, pair, keep, cut]
            spins[pair, a, keep, NEV:PAIR] = tau[1, pair, keep, cut]
        for q in range(2):
            for a in range(SPIN):
                into = perm_ref[q, a]
                sign = (2 * sign_ref[q, a] - 1) * jnp.where(into < SPIN // 2, 1, -1)
                block = spins[pair, into, keep, :] * sign.astype(F32).astype(BF16)
                moved[pair, q, 0, keep, a * NEV : (a + 1) * NEV] = block[:, 0:NEV]
                moved[pair, q, 1, keep, a * NEV : (a + 1) * NEV] = block[:, NEV:PAIR]
            real, imag = moved[pair, q, 0, keep, :], moved[pair, q, 1, keep, :]
            moved[pair, q, 2, keep, :] = (real.astype(F32) - imag.astype(F32)).astype(BF16)


def close_rows(pair, start, rows, table, spins, moved, mixed, out_ref, before):
    for a in range(SPIN):
        product = dot(spins[pair, a, pl.ds(start, rows), :], table[...])
        real, imag = product[:, 0:PAIR], product[:, PAIR:NDIM]
        for c, value in enumerate((real, imag, real + imag)):
            value = value.astype(BF16)
            for q in range(2):
                mixed[q, c, :, a * NEV : (a + 1) * NEV] = value[:, q * NEV : (q + 1) * NEV]
    keep = pl.ds(start, rows)

    @pl.loop(0, 2)
    def _(q):
        before(q)
        for left in range(0, NDIM, WIDTH):
            cols = slice(left, left + WIDTH)
            first = dot(mixed[q, 0], moved[pair, q, 0, cols], NT)
            second = dot(mixed[q, 1], moved[pair, q, 1, cols], NT)
            third = dot(mixed[q, 2], moved[pair, q, 2, cols], NT)
            out_ref[q, 0, pair, keep, cols] = (first + second).astype(BF16)
            imag = third - first + second
            out_ref[q, 1, pair, keep, cols] = imag.astype(BF16)
            out_ref[q, 2, pair, keep, cols] = (first + second + imag).astype(BF16)


def main_kernel(
    count, cuts, rows,
    mom_hbm, perm_hbm, sign_hbm, site_hbm, vec_hbm, tau_hbm,
    out_ref, sink_ref,
    mom_ref, perm_ref, sign_ref, site_ref, phase, vecs, turned, acc, tau, spins, moved, mixed, part, held, whole, table,
    small_sem, vec_sem, tau_sem, send_sem, recv_sem, back_send, back_recv, sink_send, sink_recv,
):
    time, me = lax.axis_index("ta"), lax.axis_index("gx")
    depth, lanes = vecs.shape[0], vecs.shape[-1]
    chunks = COLOR * cuts
    small = ((mom_hbm, mom_ref), (site_hbm, site_ref), (perm_hbm, perm_ref), (sign_hbm, sign_ref))
    small = [pltpu.make_async_copy(a, b, small_sem.at[k]) for k, (a, b) in enumerate(small)]

    def fetch(i):
        span = pl.ds(pl.multiple_of(lax.rem(i, cuts) * lanes, lanes), lanes)
        turn = lax.rem(i, depth)
        return pltpu.make_async_copy(vec_hbm.at[:, i // cuts, :, span], vecs.at[turn], vec_sem.at[turn])

    for copy in small:
        copy.start()
    for i in range(depth):
        fetch(i).start()
    fetch_tau = pltpu.make_async_copy(tau_hbm, tau, tau_sem)
    fetch_tau.start()

    slot = lax.rem(time, 2)
    sibling = {"ta": time + 1 - 2 * slot}
    barrier = pltpu.get_barrier_semaphore()
    for hop in range(1, count):
        pl.semaphore_signal(barrier, inc=1, device_id={"gx": lax.rem(me + hop, count)}, device_id_type=MESH)
    source = {"ta": 2 * me + slot, "gx": look_up(SOURCE, me, time // 2)}
    pl.semaphore_signal(barrier, inc=1, device_id=source, device_id_type=MESH)
    pl.semaphore_signal(barrier, inc=1, device_id=sibling, device_id_type=MESH)

    small[0].wait()
    small[1].wait()
    load_phases(mom_ref, site_ref, phase)
    fetch(0).wait()
    acc[...] = jnp.zeros_like(acc)

    @pl.loop(0, chunks)
    def _(i):
        @pl.when(i > 0)
        def _():
            fetch(i).wait()

        own = vecs.at[lax.rem(i, depth)]
        turn_chunk(own, phase, lax.rem(i, cuts), turned, lanes)
        plain = jnp.concatenate([own[0], own[1]], axis=0)
        acc[...] += dot(plain, turned[...], NT)

        @pl.when(i + depth < chunks)
        def _():
            fetch(i + depth).start()

    small[2].wait()
    small[3].wait()

    norm = 0.5 / math.sqrt(COLOR * SITES * NEV)
    half = count // 2
    width = PAIR // count
    real = (acc[0:NEV, 0:PAIR] + acc[NEV:PAIR, PAIR:NDIM]) * norm
    imag = (acc[0:NEV, PAIR:NDIM] - acc[NEV:PAIR, 0:PAIR]) * norm
    part[0:half] = real.astype(BF16).reshape(half, width, PAIR)
    part[half:count] = imag.astype(BF16).reshape(half, width, PAIR)

    pl.semaphore_wait(barrier, count + 1)
    copies = []
    for hop in range(1, count):
        peer = lax.rem(me + hop, count)
        copy = pltpu.make_async_remote_copy(
            src_ref=part.at[peer], dst_ref=held.at[hop],
            send_sem=send_sem.at[hop], recv_sem=recv_sem.at[hop],
            device_id={"gx": peer}, device_id_type=MESH,
        )
        copy.start()
        copies.append(copy)
    fetch_tau.wait()
    arrange(0, perm_ref, sign_ref, tau, spins, moved)
    total = part[me].astype(F32)
    for hop in range(1, count):
        copies[hop - 1].wait_recv()
        total = total + held[hop].astype(F32)
    whole[me] = total.astype(BF16)
    backs = []
    for hop in range(1, count):
        back = pltpu.make_async_remote_copy(
            src_ref=whole.at[me], dst_ref=whole.at[me],
            send_sem=back_send.at[hop], recv_sem=back_recv.at[hop],
            device_id={"gx": lax.rem(me + hop, count)}, device_id_type=MESH,
        )
        back.start()
        backs.append(back)
    arrange(1, perm_ref, sign_ref, tau, spins, moved)
    for hop in range(1, count):
        copies[hop - 1].wait_send()
        backs[hop - 1].wait()

    target = time // 2
    sink = pltpu.make_async_remote_copy(
        src_ref=whole, dst_ref=sink_ref.at[slot], send_sem=sink_send.at[0], recv_sem=sink_recv.at[0],
        device_id={"ta": 2 * look_up(TARGET, target, me) + slot, "gx": target}, device_id_type=MESH,
    )
    sink.start()

    first = whole[0:half].reshape(NEV, PAIR)
    second = whole[half:count].reshape(NEV, PAIR)
    table[0:NEV, 0:PAIR] = first
    table[0:NEV, PAIR:NDIM] = second
    table[NEV:PAIR, 0:PAIR] = -second
    table[NEV:PAIR, PAIR:NDIM] = first

    blocks = NDIM // rows
    last = 2 * blocks - 1
    onward = pltpu.make_async_remote_copy(
        src_ref=sink_ref.at[slot], dst_ref=sink_ref.at[slot], send_sem=sink_send.at[1], recv_sem=sink_recv.at[1],
        device_id=sibling, device_id_type=MESH,
    )

    @pl.loop(0, last + 1)
    def _(i):
        def before(q):
            @pl.when((i == last) & (q == 1))
            def _():
                sink.wait_recv()
                onward.start()

        start = pl.multiple_of(lax.rem(i, blocks) * rows, rows)
        close_rows(i // blocks, start, rows, table, spins, moved, mixed, out_ref, before)

    sink.wait_send()
    onward.wait()


def pinned(array):
    return pltpu.with_memory_space_constraint(array, pltpu.HBM)


def main_call(momenta, spin_perm, spin_sign, site_index, vectors, peram, count, chunk=2048, rows=384):
    sites = vectors.shape[-1]
    cuts = sites // chunk
    width = PAIR // count
    vmem = pl.BlockSpec(memory_space=pltpu.VMEM)
    hbm = pl.BlockSpec(memory_space=pltpu.HBM)
    dma = pltpu.SemaphoreType.DMA
    return pl.pallas_call(
        functools.partial(main_kernel, count, cuts, rows),
        out_shape=(
            pltpu.VMEM((2, 3, 2, NDIM, NDIM), BF16),
            pltpu.VMEM((2, count, width, PAIR), BF16),
        ),
        in_specs=[hbm] * 6,
        out_specs=(vmem, vmem),
        scratch_shapes=[
            pltpu.SMEM(momenta.shape, jnp.int32),
            pltpu.SMEM(spin_perm.shape, jnp.int32),
            pltpu.SMEM(spin_sign.shape, jnp.int32),
            pltpu.VMEM((cuts, chunk // LANE, LANE), jnp.int32),
            pltpu.VMEM((4, cuts, chunk // LANE, 8, LANE), F32),
            pltpu.VMEM((DEPTH, 2, NEV, chunk), BF16),
            pltpu.VMEM((NDIM, chunk), BF16),
            pltpu.VMEM((PAIR, NDIM), F32),
            pltpu.VMEM((2, 2, NDIM, NDIM), BF16),
            pltpu.VMEM((2, SPIN, NDIM, PAIR), BF16),
            pltpu.VMEM((2, 2, 3, NDIM, NDIM), BF16),
            pltpu.VMEM((2, 3, rows, NDIM), BF16),
            pltpu.VMEM((count, width, PAIR), BF16),
            pltpu.VMEM((count, width, PAIR), BF16),
            pltpu.VMEM((count, width, PAIR), BF16),
            pltpu.VMEM((PAIR, NDIM), BF16),
            dma((4,)),
            dma((DEPTH,)),
            dma,
            dma((count,)),
            dma((count,)),
            dma((count,)),
            dma((count,)),
            dma((2,)),
            dma((2,)),
        ],
        compiler_params=pltpu.CompilerParams(
            collective_id=0, has_side_effects=True, vmem_limit_bytes=45 * 1024 * 1024
        ),
        name="project_sum_close",
    )(*map(pinned, (momenta, spin_perm, spin_sign, site_index.reshape(cuts, chunk // LANE, LANE), vectors, peram)))


def apply_kernel(group, perm_hbm, sign_hbm, elem_ref, x_ref, out0_hbm, out1_hbm, perm_ref, sign_ref, table, stage, small_sem, out_sem):
    sinks = x_ref.shape[2]
    parts = SPIN // group
    small = [
        pltpu.make_async_copy(perm_hbm, perm_ref, small_sem.at[0]),
        pltpu.make_async_copy(sign_hbm, sign_ref, small_sem.at[1]),
    ]
    for copy in small:
        copy.start()

    @pl.loop(0, 2 * sinks)
    def _(n):
        pair, d = n // 2, lax.rem(n, 2)
        both_real, both_imag = elem_ref[pair, 0:NEV], elem_ref[pair, NEV:PAIR]
        real = jnp.where(d == 0, both_real[:, 0:NEV], both_real[:, NEV:PAIR])
        imag = jnp.where(d == 0, both_imag[:, 0:NEV], both_imag[:, NEV:PAIR])
        table[n, 0] = real
        table[n, 1] = imag
        table[n, 2] = (real.astype(F32) + imag.astype(F32)).astype(BF16)

    for copy in small:
        copy.wait()
    chiral = jnp.where(lax.broadcasted_iota(jnp.int32, (1, NDIM), 1) < NDIM // 2, 1.0, -1.0)
    weights = chiral * (0.5 / math.sqrt(NDIM))
    steps = sinks * 2 * parts

    def where(i):
        n, part = i // parts, lax.rem(i, parts)
        return n, n // 2, lax.rem(n, 2), part, lax.rem(i, 2)

    def store(i, out_hbm):
        n, pair, d, part, slot = where(i)
        keep = pl.ds(pl.multiple_of(part * group * NEV, group * NEV), group * NEV)
        return pltpu.make_async_copy(stage.at[slot], out_hbm.at[:, pair, 0, keep, :], out_sem.at[slot])

    @pl.loop(0, steps)
    def _(i):
        n, pair, d, part, slot = where(i)

        @pl.when(i >= 2)
        def _():
            store(i, out0_hbm).wait()

        for r in range(group):
            span = pl.ds(pl.multiple_of(perm_ref[d, part * group + r] * NEV, NEV), NEV)
            signed = weights * (2 * sign_ref[d, part * group + r] - 1).astype(F32)
            rows = slice(r * NEV, (r + 1) * NEV)
            for left in range(0, NDIM, WIDTH):
                cols = slice(left, left + WIDTH)
                first = dot(table[n, 0], x_ref[1 - d, 0, pair, span, cols])
                second = dot(table[n, 1], x_ref[1 - d, 1, pair, span, cols])
                third = dot(table[n, 2], x_ref[1 - d, 2, pair, span, cols])
                stage[slot, 0, rows, cols] = ((first - second) * signed[:, cols]).astype(BF16)
                stage[slot, 1, rows, cols] = ((third - first - second) * signed[:, cols]).astype(BF16)

        @pl.when(d == 0)
        def _():
            store(i, out0_hbm).start()

        @pl.when(d == 1)
        def _():
            store(i, out1_hbm).start()

    for i in (steps - 2, steps - 1):
        store(i, out0_hbm).wait()


def apply_sinks(elem, blocks, spin_perm, spin_sign, group=4, interpret=False):
    sinks = blocks.shape[2]
    shape = jax.ShapeDtypeStruct((2, sinks, 1, NDIM, NDIM), BF16)
    vmem = pl.BlockSpec(memory_space=pltpu.VMEM)
    hbm = pl.BlockSpec(memory_space=pltpu.HBM)
    return pl.pallas_call(
        functools.partial(apply_kernel, group),
        out_shape=(shape, shape),
        in_specs=[hbm, hbm, vmem, vmem],
        out_specs=(hbm, hbm),
        scratch_shapes=[
            pltpu.SMEM(spin_perm.shape, jnp.int32),
            pltpu.SMEM(spin_sign.shape, jnp.int32),
            pltpu.VMEM((2 * sinks, 3, NEV, NEV), BF16),
            pltpu.VMEM((2, 2, group * NEV, NDIM), BF16),
            pltpu.SemaphoreType.DMA((2,)),
            pltpu.SemaphoreType.DMA((2,)),
        ],
        compiler_params=pltpu.CompilerParams(vmem_limit_bytes=24 * 1024 * 1024),
        name="apply_sinks",
        interpret=interpret,
    )(pinned(spin_perm), pinned(spin_sign), elem, blocks)


def on_device(count, eigenvectors, site_index, momenta, perambulators, spin_perm, spin_sign):
    vectors = jnp.transpose(eigenvectors[0], (0, 2, 3, 1))
    blocks, elem = main_call(
        momenta, spin_perm, spin_sign, site_index, vectors, perambulators[:, :, 0], count
    )
    return apply_sinks(elem.reshape(2, PAIR, PAIR), blocks, spin_perm, spin_sign)


def solution(mesh):
    return jax.shard_map(
        functools.partial(on_device, mesh.shape["gx"]),
        mesh=mesh,
        in_specs=(
            P("ta", None, "gx", None, None),
            P("gx"),
            P(),
            P(None, "gx", "ta", None, None),
            P(),
            P(),
        ),
        out_specs=(P(None, "gx", "ta", None, None), P(None, "gx", "ta", None, None)),
        check_vma=False,
    )
```

```python
import functools
import math

import jax
import jax.numpy as jnp
from jax import lax
from jax.experimental import pallas as pl
from jax.experimental.pallas import tpu as pltpu
from jax.sharding import PartitionSpec as P

L = 32
NEV = 192
COLOR = 3
SPIN = 4
SITES = 32768
NDIM = SPIN * NEV
PAIR = 2 * NEV
LANE = 128
WIDTH = 256
DEPTH = 3
MESH = pl.DeviceIdType.MESH
F32 = jnp.float32
BF16 = jnp.bfloat16
NT = (((1,), (1,)), ((), ()))
NN = (((1,), (0,)), ((), ()))


def dot(a, b, dims=NN):
    return lax.dot_general(a, b, dims, preferred_element_type=F32)


FIRST = (3, 5, 6, 0, 2, 4, 7, 1)
TWIST = (0, 2, 6, 4, 5, 7, 3, 1)
SOURCE = [[a ^ b for a in FIRST] for b in TWIST]
TARGET = [[row.index(chip) for chip in range(8)] for row in SOURCE]


def look_up(table, i, j):
    found = 0
    for a, row in enumerate(table):
        for b, value in enumerate(row):
            found = found + jnp.where((i == a) & (j == b), value, 0)
    return found


def load_phases(mom_ref, site_ref, phase):
    site = site_ref[...]
    first, second, third = site >> 10, (site >> 5) & (L - 1), site & (L - 1)
    for p in range(2):
        dotted = mom_ref[p, 0] * first + mom_ref[p, 1] * second + mom_ref[p, 2] * third
        angle = (dotted & (L - 1)).astype(F32) * (2.0 * math.pi / L)
        for k, value in enumerate((jnp.cos(angle), jnp.sin(angle))):
            phase[2 * p + k] = jnp.broadcast_to(value[:, :, None, :], value.shape[:2] + (8, LANE))


def turn_chunk(vec, phase, cut, turned, lanes):
    for j in range(lanes // LANE):
        span = slice(j * LANE, (j + 1) * LANE)
        real = vec[0, :, span].astype(F32).reshape(NEV // 8, 8, LANE)
        imag = vec[1, :, span].astype(F32).reshape(NEV // 8, 8, LANE)
        for p in range(2):
            cosine = phase[2 * p, cut, j][None]
            sine = phase[2 * p + 1, cut, j][None]
            first = (cosine * real - sine * imag).reshape(NEV, LANE)
            second = (cosine * imag + sine * real).reshape(NEV, LANE)
            turned[p * NEV : (p + 1) * NEV, span] = first.astype(BF16)
            turned[PAIR + p * NEV : PAIR + (p + 1) * NEV, span] = second.astype(BF16)


def arrange(pair, perm_ref, sign_ref, tau, spins, moved, rows=128):
    @pl.loop(0, NDIM // rows)
    def _(i):
        keep = pl.ds(pl.multiple_of(i * rows, rows), rows)
        for a in range(SPIN):
            cut = slice(a * NEV, (a + 1) * NEV)
            spins[pair, a, keep, 0:NEV] = tau[0, pair, keep, cut]
            spins[pair, a, keep, NEV:PAIR] = tau[1, pair, keep, cut]
        for q in range(2):
            for a in range(SPIN):
                into = perm_ref[q, a]
                sign = (2 * sign_ref[q, a] - 1) * jnp.where(into < SPIN // 2, 1, -1)
                block = spins[pair, into, keep, :] * sign.astype(F32).astype(BF16)
                moved[pair, q, 0, keep, a * NEV : (a + 1) * NEV] = block[:, 0:NEV]
                moved[pair, q, 1, keep, a * NEV : (a + 1) * NEV] = block[:, NEV:PAIR]
            real, imag = moved[pair, q, 0, keep, :], moved[pair, q, 1, keep, :]
            moved[pair, q, 2, keep, :] = (real.astype(F32) - imag.astype(F32)).astype(BF16)


def close_rows(pair, start, rows, table, spins, moved, mixed, out_ref, before):
    for a in range(SPIN):
        product = dot(spins[pair, a, pl.ds(start, rows), :], table[...])
        real, imag = product[:, 0:PAIR], product[:, PAIR:NDIM]
        for c, value in enumerate((real, imag, real + imag)):
            value = value.astype(BF16)
            for q in range(2):
                mixed[q, c, :, a * NEV : (a + 1) * NEV] = value[:, q * NEV : (q + 1) * NEV]
    keep = pl.ds(start, rows)

    for q in range(2):
        before(q)
        for left in range(0, NDIM, WIDTH):
            cols = slice(left, left + WIDTH)
            first = dot(mixed[q, 0], moved[pair, q, 0, cols], NT)
            second = dot(mixed[q, 1], moved[pair, q, 1, cols], NT)
            third = dot(mixed[q, 2], moved[pair, q, 2, cols], NT)
            out_ref[q, 0, pair, keep, cols] = (first + second).astype(BF16)
            imag = third - first + second
            out_ref[q, 1, pair, keep, cols] = imag.astype(BF16)
            out_ref[q, 2, pair, keep, cols] = (first + second + imag).astype(BF16)


def main_kernel(
    count, cuts, rows,
    mom_hbm, perm_hbm, sign_hbm, site_hbm, vec_hbm, tau_hbm,
    out_ref, sink_ref,
    mom_ref, perm_ref, sign_ref, site_ref, phase, vecs, turned, acc, tau, spins, moved, mixed, part, held, whole, table,
    small_sem, vec_sem, tau_sem, send_sem, recv_sem, back_send, back_recv, sink_send, sink_recv,
):
    time, me = lax.axis_index("ta"), lax.axis_index("gx")
    depth, lanes = vecs.shape[0], vecs.shape[-1]
    chunks = COLOR * cuts
    small = ((mom_hbm, mom_ref), (site_hbm, site_ref), (perm_hbm, perm_ref), (sign_hbm, sign_ref))
    small = [pltpu.make_async_copy(a, b, small_sem.at[k]) for k, (a, b) in enumerate(small)]

    def fetch(i):
        span = pl.ds(pl.multiple_of(lax.rem(i, cuts) * lanes, lanes), lanes)
        turn = lax.rem(i, depth)
        return pltpu.make_async_copy(vec_hbm.at[:, i // cuts, :, span], vecs.at[turn], vec_sem.at[turn])

    fetch(0).start()
    for copy in small:
        copy.start()
    fetch_tau = pltpu.make_async_copy(tau_hbm, tau, tau_sem)

    slot = lax.rem(time, 2)
    sibling = {"ta": time + 1 - 2 * slot}
    barrier = pltpu.get_barrier_semaphore()
    for hop in range(1, count):
        pl.semaphore_signal(barrier, inc=1, device_id={"gx": lax.rem(me + hop, count)}, device_id_type=MESH)
    source = {"ta": 2 * me + slot, "gx": look_up(SOURCE, me, time // 2)}
    pl.semaphore_signal(barrier, inc=1, device_id=source, device_id_type=MESH)
    pl.semaphore_signal(barrier, inc=1, device_id=sibling, device_id_type=MESH)

    small[0].wait()
    small[1].wait()
    load_phases(mom_ref, site_ref, phase)
    fetch(0).wait()
    for i in range(1, depth):
        fetch(i).start()
    fetch_tau.start()
    acc[...] = jnp.zeros_like(acc)

    @pl.loop(0, chunks)
    def _(i):
        @pl.when(i > 0)
        def _():
            fetch(i).wait()

        own = vecs.at[lax.rem(i, depth)]
        turn_chunk(own, phase, lax.rem(i, cuts), turned, lanes)
        plain = jnp.concatenate([own[0], own[1]], axis=0)
        acc[...] += dot(plain, turned[...], NT)

        @pl.when(i + depth < chunks)
        def _():
            fetch(i + depth).start()

    small[2].wait()
    small[3].wait()

    norm = 0.5 / math.sqrt(COLOR * SITES * NEV)
    half = count // 2
    width = PAIR // count
    real = (acc[0:NEV, 0:PAIR] + acc[NEV:PAIR, PAIR:NDIM]) * norm
    imag = (acc[0:NEV, PAIR:NDIM] - acc[NEV:PAIR, 0:PAIR]) * norm
    part[0:half] = real.astype(BF16).reshape(half, width, PAIR)
    part[half:count] = imag.astype(BF16).reshape(half, width, PAIR)

    pl.semaphore_wait(barrier, count + 1)
    copies = []
    for hop in range(1, count):
        peer = lax.rem(me + hop, count)
        copy = pltpu.make_async_remote_copy(
            src_ref=part.at[peer], dst_ref=held.at[hop],
            send_sem=send_sem.at[hop], recv_sem=recv_sem.at[hop],
            device_id={"gx": peer}, device_id_type=MESH,
        )
        copy.start()
        copies.append(copy)
    fetch_tau.wait()
    arrange(0, perm_ref, sign_ref, tau, spins, moved)
    total = part[me].astype(F32)
    for hop in range(1, count):
        copies[hop - 1].wait_recv()
        total = total + held[hop].astype(F32)
    whole[me] = total.astype(BF16)
    backs = []
    for hop in range(1, count):
        back = pltpu.make_async_remote_copy(
            src_ref=whole.at[me], dst_ref=whole.at[me],
            send_sem=back_send.at[hop], recv_sem=back_recv.at[hop],
            device_id={"gx": lax.rem(me + hop, count)}, device_id_type=MESH,
        )
        back.start()
        backs.append(back)
    arrange(1, perm_ref, sign_ref, tau, spins, moved)
    for hop in range(1, count):
        copies[hop - 1].wait_send()
        backs[hop - 1].wait()

    target = time // 2
    sink = pltpu.make_async_remote_copy(
        src_ref=whole, dst_ref=sink_ref.at[slot], send_sem=sink_send.at[0], recv_sem=sink_recv.at[0],
        device_id={"ta": 2 * look_up(TARGET, target, me) + slot, "gx": target}, device_id_type=MESH,
    )
    sink.start()

    first = whole[0:half].reshape(NEV, PAIR)
    second = whole[half:count].reshape(NEV, PAIR)
    table[0:NEV, 0:PAIR] = first
    table[0:NEV, PAIR:NDIM] = second
    table[NEV:PAIR, 0:PAIR] = -second
    table[NEV:PAIR, PAIR:NDIM] = first

    blocks = NDIM // rows
    last = 2 * blocks - 1
    onward = pltpu.make_async_remote_copy(
        src_ref=sink_ref.at[slot], dst_ref=sink_ref.at[slot], send_sem=sink_send.at[1], recv_sem=sink_recv.at[1],
        device_id=sibling, device_id_type=MESH,
    )

    @pl.loop(0, last + 1)
    def _(i):
        def before(q):
            if q == 1:
                @pl.when(i == last)
                def _():
                    sink.wait_recv()
                    onward.start()

        start = pl.multiple_of(lax.rem(i, blocks) * rows, rows)
        close_rows(i // blocks, start, rows, table, spins, moved, mixed, out_ref, before)

    sink.wait_send()
    onward.wait()


def pinned(array):
    return pltpu.with_memory_space_constraint(array, pltpu.HBM)


def main_call(momenta, spin_perm, spin_sign, site_index, vectors, peram, count, chunk=2048, rows=384):
    sites = vectors.shape[-1]
    cuts = sites // chunk
    width = PAIR // count
    vmem = pl.BlockSpec(memory_space=pltpu.VMEM)
    hbm = pl.BlockSpec(memory_space=pltpu.HBM)
    dma = pltpu.SemaphoreType.DMA
    return pl.pallas_call(
        functools.partial(main_kernel, count, cuts, rows),
        out_shape=(
            pltpu.VMEM((2, 3, 2, NDIM, NDIM), BF16),
            pltpu.VMEM((2, count, width, PAIR), BF16),
        ),
        in_specs=[hbm] * 6,
        out_specs=(vmem, vmem),
        scratch_shapes=[
            pltpu.SMEM(momenta.shape, jnp.int32),
            pltpu.SMEM(spin_perm.shape, jnp.int32),
            pltpu.SMEM(spin_sign.shape, jnp.int32),
            pltpu.VMEM((cuts, chunk // LANE, LANE), jnp.int32),
            pltpu.VMEM((4, cuts, chunk // LANE, 8, LANE), F32),
            pltpu.VMEM((DEPTH, 2, NEV, chunk), BF16),
            pltpu.VMEM((NDIM, chunk), BF16),
            pltpu.VMEM((PAIR, NDIM), F32),
            pltpu.VMEM((2, 2, NDIM, NDIM), BF16),
            pltpu.VMEM((2, SPIN, NDIM, PAIR), BF16),
            pltpu.VMEM((2, 2, 3, NDIM, NDIM), BF16),
            pltpu.VMEM((2, 3, rows, NDIM), BF16),
            pltpu.VMEM((count, width, PAIR), BF16),
            pltpu.VMEM((count, width, PAIR), BF16),
            pltpu.VMEM((count, width, PAIR), BF16),
            pltpu.VMEM((PAIR, NDIM), BF16),
            dma((4,)),
            dma((DEPTH,)),
            dma,
            dma((count,)),
            dma((count,)),
            dma((count,)),
            dma((count,)),
            dma((2,)),
            dma((2,)),
        ],
        compiler_params=pltpu.CompilerParams(
            collective_id=0, has_side_effects=True, vmem_limit_bytes=45 * 1024 * 1024
        ),
        name="project_sum_close",
    )(*map(pinned, (momenta, spin_perm, spin_sign, site_index.reshape(cuts, chunk // LANE, LANE), vectors, peram)))


def apply_kernel(group, perm_hbm, sign_hbm, elem_ref, x_ref, out0_hbm, out1_hbm, perm_ref, sign_ref, table, stage, small_sem, out_sem):
    sinks = x_ref.shape[2]
    parts = SPIN // group
    small = [
        pltpu.make_async_copy(perm_hbm, perm_ref, small_sem.at[0]),
        pltpu.make_async_copy(sign_hbm, sign_ref, small_sem.at[1]),
    ]
    for copy in small:
        copy.start()

    @pl.loop(0, 2 * sinks)
    def _(n):
        pair, d = n // 2, lax.rem(n, 2)
        both_real, both_imag = elem_ref[pair, 0:NEV], elem_ref[pair, NEV:PAIR]
        real = jnp.where(d == 0, both_real[:, 0:NEV], both_real[:, NEV:PAIR])
        imag = jnp.where(d == 0, both_imag[:, 0:NEV], both_imag[:, NEV:PAIR])
        table[n, 0] = real
        table[n, 1] = imag
        table[n, 2] = (real.astype(F32) + imag.astype(F32)).astype(BF16)

    for copy in small:
        copy.wait()
    chiral = jnp.where(lax.broadcasted_iota(jnp.int32, (1, NDIM), 1) < NDIM // 2, 1.0, -1.0)
    weights = chiral * (0.5 / math.sqrt(NDIM))
    steps = sinks * 2 * parts

    def where(i):
        n, part = i // parts, lax.rem(i, parts)
        return n, n // 2, lax.rem(n, 2), part, lax.rem(i, 2)

    def store(i, out_hbm):
        n, pair, d, part, slot = where(i)
        keep = pl.ds(pl.multiple_of(part * group * NEV, group * NEV), group * NEV)
        return pltpu.make_async_copy(stage.at[slot], out_hbm.at[:, pair, 0, keep, :], out_sem.at[slot])

    @pl.loop(0, steps)
    def _(i):
        n, pair, d, part, slot = where(i)

        @pl.when(i >= 2)
        def _():
            store(i, out0_hbm).wait()

        for r in range(group):
            span = pl.ds(pl.multiple_of(perm_ref[d, part * group + r] * NEV, NEV), NEV)
            signed = weights * (2 * sign_ref[d, part * group + r] - 1).astype(F32)
            rows = slice(r * NEV, (r + 1) * NEV)
            for left in range(0, NDIM, WIDTH):
                cols = slice(left, left + WIDTH)
                first = dot(table[n, 0], x_ref[1 - d, 0, pair, span, cols])
                second = dot(table[n, 1], x_ref[1 - d, 1, pair, span, cols])
                third = dot(table[n, 2], x_ref[1 - d, 2, pair, span, cols])
                stage[slot, 0, rows, cols] = ((first - second) * signed[:, cols]).astype(BF16)
                stage[slot, 1, rows, cols] = ((third - first - second) * signed[:, cols]).astype(BF16)

        @pl.when(d == 0)
        def _():
            store(i, out0_hbm).start()

        @pl.when(d == 1)
        def _():
            store(i, out1_hbm).start()

    for i in (steps - 2, steps - 1):
        store(i, out0_hbm).wait()


def apply_sinks(elem, blocks, spin_perm, spin_sign, group=4, interpret=False):
    sinks = blocks.shape[2]
    shape = jax.ShapeDtypeStruct((2, sinks, 1, NDIM, NDIM), BF16)
    vmem = pl.BlockSpec(memory_space=pltpu.VMEM)
    hbm = pl.BlockSpec(memory_space=pltpu.HBM)
    return pl.pallas_call(
        functools.partial(apply_kernel, group),
        out_shape=(shape, shape),
        in_specs=[hbm, hbm, vmem, vmem],
        out_specs=(hbm, hbm),
        scratch_shapes=[
            pltpu.SMEM(spin_perm.shape, jnp.int32),
            pltpu.SMEM(spin_sign.shape, jnp.int32),
            pltpu.VMEM((2 * sinks, 3, NEV, NEV), BF16),
            pltpu.VMEM((2, 2, group * NEV, NDIM), BF16),
            pltpu.SemaphoreType.DMA((2,)),
            pltpu.SemaphoreType.DMA((2,)),
        ],
        compiler_params=pltpu.CompilerParams(vmem_limit_bytes=24 * 1024 * 1024),
        name="apply_sinks",
        interpret=interpret,
    )(pinned(spin_perm), pinned(spin_sign), elem, blocks)


def on_device(count, eigenvectors, site_index, momenta, perambulators, spin_perm, spin_sign):
    vectors = jnp.transpose(eigenvectors[0], (0, 2, 3, 1))
    blocks, elem = main_call(
        momenta, spin_perm, spin_sign, site_index, vectors, perambulators[:, :, 0], count
    )
    return apply_sinks(elem.reshape(2, PAIR, PAIR), blocks, spin_perm, spin_sign)


def solution(mesh):
    return jax.shard_map(
        functools.partial(on_device, mesh.shape["gx"]),
        mesh=mesh,
        in_specs=(
            P("ta", None, "gx", None, None),
            P("gx"),
            P(),
            P(None, "gx", "ta", None, None),
            P(),
            P(),
        ),
        out_specs=(P(None, "gx", "ta", None, None), P(None, "gx", "ta", None, None)),
        check_vma=False,
    )
```
